32 devices in a mesh: data: 32 (over z, y, x, core).
Axes of the slice: x: 2, y: 2, z: 4, core: 2. Of those that a mesh axis runs over, the one named last changes fastest.
Arguments:
- grad_attn: bfloat16 [32, 16, 262144], P('data')
- grad_mlp: bfloat16 [32, 8, 1048576], P('data')
- grad_wide: bfloat16 [32, 4, 2048], P('data')
- grad_vec: bfloat16 [32, 38, 512], P('data')
- weight_attn: float32 [16, 262144], P(None, 'data')
- weight_mlp: float32 [8, 1048576], P(None, 'data')
- weight_wide: float32 [4, 2048], P(None, 'data')
- weight_vec: float32 [38, 512], P(None, 'data')
- mom1_attn: float32 [16, 262144], P(None, 'data')
- mom1_mlp: float32 [8, 1048576], P(None, 'data')
- mom1_wide: float32 [4, 2048], P(None, 'data')
- mom1_vec: float32 [38, 512], P(None, 'data')
- mom2_attn: float32 [16, 262144], P(None, 'data')
- mom2_mlp: float32 [8, 1048576], P(None, 'data')
- mom2_wide: float32 [4, 2048], P(None, 'data')
- mom2_vec: float32 [38, 512], P(None, 'data')
Outputs:
- output 1: bfloat16 [16, 262144], replicated
- output 2: bfloat16 [8, 1048576], replicated
- output 3: bfloat16 [4, 2048], replicated
- output 4: bfloat16 [38, 512], replicated
- output 5: float32 [16, 262144], P(None, 'data')
- output 6: float32 [8, 1048576], P(None, 'data')
- output 7: float32 [4, 2048], P(None, 'data')
- output 8: float32 [38, 512], P(None, 'data')
- output 9: float32 [16, 262144], P(None, 'data')
- output 10: float32 [8, 1048576], P(None, 'data')
- output 11: float32 [4, 2048], P(None, 'data')
- output 12: float32 [38, 512], P(None, 'data')
- output 13: float32 [16, 262144], P(None, 'data')
- output 14: float32 [8, 1048576], P(None, 'data')
- output 15: float32 [4, 2048], P(None, 'data')
- output 16: float32 [38, 512], P(None, 'data')
All inputs are finite; a program needn't handle non-finite values.
Results may differ from the reference program's by a relative error of at most 0.001.
Values are sent between devices in bfloat16 or wider.
A program may use at most 1 GiB of HBM per device.

```python
import jax
import jax.numpy as jnp

GROUP_SIZE = 32
LAYERS = 4
D = 512
FF = 2048
STEP_NUMBER = 10

LEARN_RATE = 0.04
BETA_FIRST = 0.9
BETA_SECOND = 0.999
EPSILON = 1e-6
WEIGHT_DECAY = 0.01
MAX_NORM = 1.0
TARGET_NORM = 3.0


def bank_layout():
    gain_rows = jnp.array([1.0, 0.0, 0.0, 0.0, 0.0, 0.0, 1.0, 0.0, 0.0] * LAYERS + [1.0, 0.0])
    counts = (4 * LAYERS, 2 * LAYERS, LAYERS, 9 * LAYERS + 2)
    lengths = (D * D, D * FF, FF, D)
    base_scales = (
        jnp.full((4 * LAYERS,), D ** -0.5),
        jnp.array([D ** -0.5, FF ** -0.5] * LAYERS),
        jnp.full((LAYERS,), 0.05),
        0.05 + 0.15 * gain_rows,
    )
    offsets = (jnp.zeros((4 * LAYERS,)), jnp.zeros((2 * LAYERS,)), jnp.zeros((LAYERS,)), gain_rows)
    return counts, lengths, base_scales, offsets


def setup_inputs(seed: int = 0) -> dict:
    root_key = jax.random.key(seed)
    counts, lengths, base_scales, offsets = bank_layout()
    bank_keys = [jax.random.split(jax.random.fold_in(root_key, bank_index), 6) for bank_index in range(4)]
    grad_mults = [jnp.exp(jax.random.uniform(bank_keys[bank_index][0], (counts[bank_index],), minval=-1.0, maxval=1.0)) for bank_index in range(4)]
    weighted = sum(lengths[bank_index] * jnp.sum(grad_mults[bank_index] ** 2) for bank_index in range(4))
    grad_unit = TARGET_NORM * jnp.sqrt(GROUP_SIZE / weighted)
    clip_guess = MAX_NORM / TARGET_NORM
    grad_banks, weights, firsts, seconds = [], [], [], []
    for bank_index in range(4):
        bank_keyset = bank_keys[bank_index]
        row_count = counts[bank_index]
        row_length = lengths[bank_index]
        grad_scale = grad_unit * grad_mults[bank_index]
        device_grads = jax.random.normal(bank_keyset[1], (GROUP_SIZE, row_count, row_length)) * grad_scale[None, :, None]
        grad_banks.append(device_grads.astype(jnp.bfloat16))
        weight_spread = jnp.exp(jax.random.uniform(bank_keyset[2], (row_count,), minval=-1.2, maxval=1.2))
        row_scale = base_scales[bank_index] * weight_spread
        weights.append(offsets[bank_index][:, None] + row_scale[:, None] * jax.random.normal(bank_keyset[3], (row_count, row_length)))
        moment_unit = clip_guess * grad_scale / GROUP_SIZE ** 0.5
        firsts.append(0.1 * moment_unit[:, None] * jax.random.normal(bank_keyset[4], (row_count, row_length)))
        seconds.append(0.001 * (moment_unit * moment_unit)[:, None] * jnp.exp(0.5 * jax.random.normal(bank_keyset[5], (row_count, row_length))))
    bank_names = ("attn", "mlp", "wide", "vec")
    inputs = {}
    for prefix, arrays in (("grad_", grad_banks), ("weight_", weights), ("mom1_", firsts), ("mom2_", seconds)):
        for bank_index in range(4):
            inputs[prefix + bank_names[bank_index]] = arrays[bank_index]
    return inputs


def lamb_bank(mean_grad, weight, first_moment, second_moment, clip_coef):
    clipped = clip_coef * mean_grad
    new_first = BETA_FIRST * first_moment + (1.0 - BETA_FIRST) * clipped
    new_second = BETA_SECOND * second_moment + (1.0 - BETA_SECOND) * (clipped * clipped)
    update = (new_first / (1.0 - BETA_FIRST ** STEP_NUMBER)) / (jnp.sqrt(new_second / (1.0 - BETA_SECOND ** STEP_NUMBER)) + EPSILON) + WEIGHT_DECAY * weight
    weight_norm = jnp.sqrt(jnp.sum(weight * weight, axis=1, keepdims=True))
    update_norm = jnp.sqrt(jnp.sum(update * update, axis=1, keepdims=True))
    new_weight = weight - LEARN_RATE * (weight_norm / update_norm) * update
    return new_weight.astype(jnp.bfloat16), new_weight, new_first, new_second


def reference(grad_attn, grad_mlp, grad_wide, grad_vec, weight_attn, weight_mlp, weight_wide, weight_vec, mom1_attn, mom1_mlp, mom1_wide, mom1_vec, mom2_attn, mom2_mlp, mom2_wide, mom2_vec):
    mean_attn = jnp.sum(grad_attn, axis=0, dtype=jnp.float32) / GROUP_SIZE
    mean_mlp = jnp.sum(grad_mlp, axis=0, dtype=jnp.float32) / GROUP_SIZE
    mean_wide = jnp.sum(grad_wide, axis=0, dtype=jnp.float32) / GROUP_SIZE
    mean_vec = jnp.sum(grad_vec, axis=0, dtype=jnp.float32) / GROUP_SIZE
    total_square = jnp.sum(mean_attn * mean_attn) + jnp.sum(mean_mlp * mean_mlp) + jnp.sum(mean_wide * mean_wide) + jnp.sum(mean_vec * mean_vec)
    clip_coef = jnp.minimum(1.0, MAX_NORM / jnp.sqrt(total_square))
    attn_out = lamb_bank(mean_attn, weight_attn, mom1_attn, mom2_attn, clip_coef)
    mlp_out = lamb_bank(mean_mlp, weight_mlp, mom1_mlp, mom2_mlp, clip_coef)
    wide_out = lamb_bank(mean_wide, weight_wide, mom1_wide, mom2_wide, clip_coef)
    vec_out = lamb_bank(mean_vec, weight_vec, mom1_vec, mom2_vec, clip_coef)
    return (attn_out[0], mlp_out[0], wide_out[0], vec_out[0], attn_out[1], mlp_out[1], wide_out[1], vec_out[1], attn_out[2], mlp_out[2], wide_out[2], vec_out[2], attn_out[3], mlp_out[3], wide_out[3], vec_out[3])
```

```python
import jax
import jax.numpy as jnp
from jax import lax
from jax.sharding import PartitionSpec as P
from jax.experimental import pallas as pl
from jax.experimental.pallas import tpu as pltpu

STEP_NUMBER = 10
LEARN_RATE = 0.04
BETA_FIRST = 0.9
BETA_SECOND = 0.999
EPSILON = 1e-6
WEIGHT_DECAY = 0.01
MAX_NORM = 1.0

CHUNKS = 16
SCRATCHES = 18
DEVICES, HALF, OTHERS = 32, 16, 31
LANES = 128
TILE = (8, 128)
CORE, X, Y, Z0, Z1 = 1, 2, 4, 8, 16
STREAMS = (
    ("mlp", 12288, 20480, (Y, X, Z0, Z1)),
    ("mlp", 0, 12288, (X, Y, Z0, Z1)),
    ("attn", 0, 8192, (Z0, X, Y, Z1)),
)
ROWS = {"attn": 16, "mlp": 8}
SHARD = {"attn": 8192, "mlp": 32768}
MESH = pl.DeviceIdType.MESH
HIGHEST = lax.Precision.HIGHEST


def loop(first, stop, body):
    lax.fori_loop(first, stop, body, 0)


def direction(grad, weight, first, second, clip):
    clipped = clip * grad
    new_first = BETA_FIRST * first + (1.0 - BETA_FIRST) * clipped
    new_second = BETA_SECOND * second + (1.0 - BETA_SECOND) * (clipped * clipped)
    update = (new_first / (1.0 - BETA_FIRST ** STEP_NUMBER)) / (jnp.sqrt(new_second / (1.0 - BETA_SECOND ** STEP_NUMBER)) + EPSILON) + WEIGHT_DECAY * weight
    return update, new_first, new_second


def fold_lanes(value):
    total = value[:, 0:LANES]
    for column in range(LANES, value.shape[1], LANES):
        total = total + value[:, column:column + LANES]
    return total


class Stream:
    def __init__(self, bank, first_column, columns, order):
        self.bank, self.first_column, self.columns, self.order = bank, first_column, columns, order
        self.reduce_order = (order[0], CORE) + order[1:]
        self.rows = ROWS[bank]
        self.width = columns // CHUNKS

    def scratch(self):
        rows, width = self.rows, self.width
        return [
            pltpu.VMEM((2, 16, rows, width), jnp.bfloat16),
            pltpu.VMEM((CHUNKS, 16, rows, width), jnp.bfloat16),
            pltpu.VMEM((2, 16, rows, width), jnp.float32),
            pltpu.VMEM((CHUNKS, 8, rows, width), jnp.float32),
            pltpu.VMEM((CHUNKS, 4, rows, width), jnp.float32),
            pltpu.VMEM((CHUNKS, 2, rows, width), jnp.float32),
            pltpu.VMEM((CHUNKS, 1, rows, width), jnp.float32),
            pltpu.VMEM((3, CHUNKS, rows, width), jnp.float32),
            pltpu.VMEM((CHUNKS, 1, rows, width), jnp.bfloat16),
            pltpu.SemaphoreType.DMA((2,)),
            pltpu.SemaphoreType.DMA((2,)),
            pltpu.SemaphoreType.DMA((5, CHUNKS)),
            pltpu.SemaphoreType.DMA((5,)),
            pltpu.SemaphoreType.DMA((4, CHUNKS)),
            pltpu.SemaphoreType.DMA,
            pltpu.SemaphoreType.DMA,
            pltpu.SemaphoreType.DMA,
            pltpu.SemaphoreType.DMA,
        ]

    def bind(self, refs):
        (self.own, self.land, self.acc, self.part8, self.part4, self.part2, self.part1, self.state, self.narrow,
         self.own_sem, self.core_send, self.recv, self.send, self.gather_recv, self.gather_sent, self.core_sent, self.core_got, self.narrow_sem) = refs


def solution(mesh):
    grad_spec = P("data", None, None)
    shard_spec = P(None, "data")
    full_spec = P(None, None)

    def kernel(*refs):
        grads = {"attn": refs[0], "mlp": refs[1]}
        grad_small = refs[2]
        states = {"attn": refs[3:6], "mlp": refs[6:9]}
        state_small = refs[9]
        replicas = {"attn": refs[10], "mlp": refs[11]}
        replica_small = refs[12]
        news = {"attn": refs[13:16], "mlp": refs[16:19]}
        new_small = refs[19]
        rest = refs[20:]
        streams = []
        for index, spec in enumerate(STREAMS):
            stream = Stream(*spec)
            stream.bind(rest[SCRATCHES * index:SCRATCHES * (index + 1)])
            streams.append(stream)
        (small_land, small_state, small_wide, norm_out, norm_land, tile_out, tile_land, square, row_attn, row_mlp,
         small_send, small_recv, norm_send, norm_recv, tile_send, tile_recv, rep_send, rep_recv, load_sem, store_sem, copy_sem) = rest[SCRATCHES * len(streams):]

        me = lax.axis_index("data")
        bit = {w: (me // w) % 2 for w in (CORE, X, Y, Z0, Z1)}
        peer = {w: me + w - 2 * w * bit[w] for w in bit}

        def owner_at(dims, rel):
            owner = bit[CORE] if CORE not in dims else 0
            for weight in reversed(dims):
                owner = owner + weight * ((bit[weight] + rel) % 2)
                rel = rel // 2
            return owner

        def columns_of(s, owner, k):
            return pl.ds(pl.multiple_of(owner * SHARD[s.bank] + s.first_column + k * s.width, LANES), s.width)

        def remote(src, dst, send_sem, recv_sem, device):
            return pltpu.make_async_remote_copy(src_ref=src, dst_ref=dst, send_sem=send_sem, recv_sem=recv_sem, device_id=(device,), device_id_type=MESH)

        def local(src, dst, sem):
            return pltpu.make_async_copy(src, dst, sem)

        def start_raw(s, k):
            slot = k % 2
            grad = grads[s.bank]

            def body(rel, carry):
                remote(grad.at[0, :, columns_of(s, owner_at(s.reduce_order, HALF + rel), k)], s.land.at[k, rel], s.send.at[0], s.recv.at[0, k], peer[s.order[0]]).start()
                local(grad.at[0, :, columns_of(s, owner_at(s.reduce_order, rel), k)], s.own.at[slot, rel], s.own_sem.at[slot]).start()
                return carry

            loop(0, 16, body)

        def add_raw(s, k):
            slot = k % 2
            local(s.own.at[slot], s.own.at[slot], s.own_sem.at[slot]).wait()
            remote(s.land.at[k], s.land.at[k], s.send.at[0], s.recv.at[0, k], peer[s.order[0]]).wait_recv()

            @pl.when(k >= 2)
            def _():
                remote(s.acc.at[slot, pl.ds(8, 8)], s.part8.at[k], s.core_send.at[slot], s.recv.at[1, k], peer[CORE]).wait_send()

            def body(rel, carry):
                s.acc[slot, rel] = s.own[slot, rel].astype(jnp.float32) + s.land[k, rel].astype(jnp.float32)
                return carry

            loop(8, 16, body)
            remote(s.acc.at[slot, pl.ds(8, 8)], s.part8.at[k], s.core_send.at[slot], s.recv.at[1, k], peer[CORE]).start()
            loop(0, 8, body)

        def add_core(s, k):
            slot = k % 2
            remote(s.acc.at[slot, pl.ds(8, 8)], s.part8.at[k], s.core_send.at[slot], s.recv.at[1, k], peer[CORE]).wait_recv()

            def body(rel, carry):
                s.part8[k, rel] = s.part8[k, rel] + s.acc[slot, rel]
                return carry

            loop(4, 8, body)
            remote(s.part8.at[k, pl.ds(4, 4)], s.part4.at[k], s.send.at[2], s.recv.at[2, k], peer[s.order[1]]).start()
            loop(0, 4, body)

        def add_step(s, k, stage):
            held, got = (s.part8, s.part4) if stage == 2 else (s.part4, s.part2)
            half = 4 if stage == 2 else 2
            nxt = s.part2 if stage == 2 else s.part1
            remote(held.at[k, pl.ds(half, half)], got.at[k], s.send.at[stage], s.recv.at[stage, k], peer[s.order[stage - 1]]).wait_recv()

            def body(rel, carry):
                got[k, rel] = got[k, rel] + held[k, rel]
                return carry

            quarter = half // 2
            loop(quarter, half, body)
            remote(got.at[k, pl.ds(quarter, quarter)], nxt.at[k], s.send.at[stage + 1], s.recv.at[stage + 1, k], peer[s.order[stage]]).start()
            loop(0, quarter, body)

        def add_last(s, k):
            remote(s.part2.at[k, pl.ds(1, 1)], s.part1.at[k], s.send.at[4], s.recv.at[4, k], peer[s.order[3]]).wait_recv()
            grad = (s.part1[k, 0] + s.part2[k, 0]) * (1.0 / 32.0)
            s.part1[k, 0] = grad
            part = fold_lanes(grad * grad)
            for row in range(0, s.rows, 8):
                square[...] += part[row:row + 8]

        def to_all(block_for, land, send_sem, recv_sem):
            def body(d, carry):
                other = (me + d) % DEVICES
                remote(block_for(other), land.at[me], send_sem, recv_sem, other).start()
                return carry

            loop(1, DEVICES, body)

        def from_all(land, send_sem, recv_sem):
            blocks = land.at[pl.ds(0, OTHERS)]
            return remote(blocks, blocks, send_sem, recv_sem, me)

        for s in streams:
            start_raw(s, 0)
        small_land[me] = grad_small[me]
        to_all(lambda other: grad_small.at[other], small_land, small_send, small_recv)
        square[...] = jnp.zeros_like(square)

        def start_state(k, carry):
            for s in streams:
                for which in range(3):
                    local(states[s.bank][which].at[:, pl.ds(pl.multiple_of(s.first_column + k * s.width, LANES), s.width)], s.state.at[which, k], load_sem).start()
            return carry

        loop(0, CHUNKS, start_state)

        def reduce_step(t, carry):
            @pl.when(jnp.logical_and(t >= 3, t < CHUNKS + 3))
            def _():
                for s in streams:
                    add_last(s, t - 3)

            @pl.when(jnp.logical_and(t >= 2, t < CHUNKS + 2))
            def _():
                for s in streams:
                    add_step(s, t - 2, 3)

            @pl.when(jnp.logical_and(t >= 1, t < CHUNKS + 1))
            def _():
                for s in streams:
                    add_step(s, t - 1, 2)

            @pl.when(t + 1 < CHUNKS)
            def _():
                for s in streams:
                    start_raw(s, t + 1)

            @pl.when(t < CHUNKS)
            def _():
                for s in streams:
                    add_raw(s, t)
                for s in streams:
                    add_core(s, t)

            return carry

        loop(0, CHUNKS + 3, reduce_step)

        from_all(small_land, small_send, small_recv).wait_recv()
        small_grad = jnp.zeros(TILE, jnp.float32)
        for d in range(DEVICES):
            small_grad = small_grad + small_land[d].astype(jnp.float32)
        small_grad = small_grad * (1.0 / 32.0)
        norm_out[...] = jnp.sum(square[...] + small_grad * small_grad, axis=0, keepdims=True)
        norm_land[me] = norm_out[...]

        to_all(lambda other: norm_out, norm_land, norm_send, norm_recv)

        for s in streams:
            local(s.state, s.state, load_sem).wait()
        row_attn[...] = jnp.zeros_like(row_attn)
        row_mlp[...] = jnp.zeros_like(row_mlp)
        rows_of = {"attn": row_attn, "mlp": row_mlp}
        for s in streams:
            def weight_rows(k, carry, s=s):
                weight = s.state[0, k]
                rows_of[s.bank][1] += fold_lanes(weight * weight)
                return carry
            loop(0, CHUNKS, weight_rows)

        from_all(norm_land, norm_send, norm_recv).wait_recv()
        total = jnp.zeros((1, LANES), jnp.float32)
        for d in range(DEVICES):
            total = total + norm_land[d]
        clip = jnp.minimum(1.0, MAX_NORM / jnp.sqrt(jnp.sum(total, axis=1, keepdims=True)))

        for s in streams:
            def move(k, carry, s=s):
                update, new_first, new_second = direction(s.part1[k, 0], s.state[0, k], s.state[1, k], s.state[2, k], clip)
                s.part1[k, 0] = update
                s.state[1, k] = new_first
                s.state[2, k] = new_second
                rows_of[s.bank][0] += fold_lanes(update * update)
                return carry
            loop(0, CHUNKS, move)
        small_weight = state_small[0]
        small_update, small_first, small_second = direction(small_grad, small_weight, state_small[1], state_small[2], clip)
        small_state[0] = small_update
        new_small[1] = small_first
        new_small[2] = small_second

        lane = lax.broadcasted_iota(jnp.int32, TILE, 1)
        source = lax.broadcasted_iota(jnp.int32, (LANES, LANES), 0)
        target = lax.broadcasted_iota(jnp.int32, (LANES, LANES), 1)
        gather_update = jnp.where(target == source // 16 + 8, 1.0, 0.0)
        gather_weight = jnp.where(target == source // 16 + 24, 1.0, 0.0)
        tile = jnp.dot(small_update * small_update, gather_update, precision=HIGHEST, preferred_element_type=jnp.float32)
        tile = tile + jnp.dot(small_weight * small_weight, gather_weight, precision=HIGHEST, preferred_element_type=jnp.float32)
        for which, base in ((0, 0), (1, 16)):
            attn_sum = jnp.sum(row_attn[which], axis=1, keepdims=True)
            mlp_sum = jnp.sum(row_mlp[which], axis=1, keepdims=True)
            tile = tile + jnp.where(lane == base, attn_sum[0:8], 0.0) + jnp.where(lane == base + 1, attn_sum[8:16], 0.0) + jnp.where(lane == base + 2, mlp_sum, 0.0)
        tile_out[...] = tile
        tile_land[me] = tile

        to_all(lambda other: tile_out, tile_land, tile_send, tile_recv)

        def start_moments(k, carry):
            for s in streams:
                for which in (1, 2):
                    local(s.state.at[which, k], news[s.bank][which].at[:, pl.ds(pl.multiple_of(s.first_column + k * s.width, LANES), s.width)], store_sem).start()
            return carry

        loop(0, CHUNKS, start_moments)
        from_all(tile_land, tile_send, tile_recv).wait_recv()
        sums = tile_land[0]
        for d in range(1, DEVICES):
            sums = sums + tile_land[d]

        def lane_column(index):
            return jnp.sum(jnp.where(lane == index, sums, 0.0), axis=1, keepdims=True)

        def scale(weight_square, update_square):
            return LEARN_RATE * (jnp.sqrt(weight_square) / jnp.sqrt(update_square))

        scale_attn = jnp.concatenate([scale(lane_column(16), lane_column(0)), scale(lane_column(17), lane_column(1))], axis=0)
        scales = {"attn": scale_attn, "mlp": scale(lane_column(18), lane_column(2))}

        row = lax.broadcasted_iota(jnp.int32, TILE, 0)

        def spread(base):
            single = jnp.where(source == target // 16 + base, 1.0, 0.0)
            wide = jnp.where(jnp.logical_and(source // 4 == target // 64 + base // 4, source < base + 8), 1.0, 0.0)
            per_sixteen = jnp.dot(sums, single, precision=HIGHEST, preferred_element_type=jnp.float32)
            per_sixty_four = jnp.dot(sums, wide, precision=HIGHEST, preferred_element_type=jnp.float32)
            return jnp.where(row < 2, per_sixty_four, per_sixteen)

        filled = row * LANES + lane < 864
        small_scale = scale(jnp.where(filled, spread(24), 1.0), jnp.where(filled, spread(8), 1.0))
        small_new = small_weight - small_scale * small_state[0]
        new_small[0] = small_new
        small_wide[...] = small_new.astype(jnp.bfloat16)

        def gather_send(s, k, j):
            out = replicas[s.bank]
            device = peer[s.order[3 - j]]
            mine = out.at[:, columns_of(s, me, k)]
            remote(s.narrow.at[k, 0], mine, s.gather_sent, s.gather_recv.at[j, k], device).start()

            def body(rel, carry):
                block = out.at[:, columns_of(s, owner_at(s.order, rel), k)]
                remote(block, block, s.gather_sent, s.gather_recv.at[j, k], device).start()
                return carry

            if j > 0:
                loop(1, 2 ** j, body)

        def gather_wait(s, k, j):
            out = replicas[s.bank].at[:, pl.ds(0, s.width * 2 ** j)]
            remote(out, out, s.gather_sent, s.gather_recv.at[j, k], me).wait_recv()

        def core_send(s, k, j):
            out = replicas[s.bank]

            def body(rel, carry):
                block = out.at[:, columns_of(s, owner_at(s.order, rel), k)]
                remote(block, block, s.core_sent, s.core_got, peer[CORE]).start()
                return carry

            loop(2 ** j, 2 ** (j + 1), body)

        def renew(s, k):
            new_weight = s.state[0, k] - scales[s.bank] * s.part1[k, 0]
            s.state[0, k] = new_weight
            s.narrow[k, 0] = new_weight.astype(jnp.bfloat16)

        def first_sends(s, k):
            out = replicas[s.bank]
            mine = out.at[:, columns_of(s, me, k)]
            gather_send(s, k, 0)
            remote(s.narrow.at[k, 0], mine, s.core_sent, s.core_got, peer[CORE]).start()
            local(s.narrow.at[k, 0], mine, s.narrow_sem).start()
            local(s.state.at[0, k], news[s.bank][0].at[:, pl.ds(pl.multiple_of(s.first_column + k * s.width, LANES), s.width)], store_sem).start()

        def gather_step(t, carry):
            @pl.when(t < CHUNKS)
            def _():
                for s in streams:
                    renew(s, t)
                for s in streams:
                    first_sends(s, t)

            for j in (1, 2, 3):
                @pl.when(jnp.logical_and(t >= j, t < CHUNKS + j))
                def _(j=j):
                    for s in streams:
                        gather_wait(s, t - j, j - 1)
                        gather_send(s, t - j, j)
                        core_send(s, t - j, j - 1)

            @pl.when(t >= 4)
            def _():
                for s in streams:
                    gather_wait(s, t - 4, 3)
                    core_send(s, t - 4, 3)

            return carry

        gather_step(0, 0)
        to_all(lambda other: small_wide, replica_small, rep_send, rep_recv)
        local(small_wide, replica_small.at[me], copy_sem).start()
        loop(1, CHUNKS + 4, gather_step)

        for s in streams:
            out = replicas[s.bank]
            half = out.at[:, pl.ds(0, 16 * s.columns)]
            remote(half, half, s.core_sent, s.core_got, me).wait()
            sent = out.at[:, pl.ds(0, 15 * s.columns)]
            remote(sent, sent, s.gather_sent, s.core_got, me).wait_send()
            local(s.narrow, s.narrow, s.narrow_sem).wait()
            remote(s.land, s.land, s.send.at[0], s.recv.at[0, 0], me).wait_send()
            for last in (CHUNKS - 2, CHUNKS - 1):
                slot = last % 2
                remote(s.acc.at[slot, pl.ds(8, 8)], s.part8.at[last], s.core_send.at[slot], s.recv.at[1, last], me).wait_send()
            for stage, part in ((2, s.part4), (3, s.part2), (4, s.part1)):
                remote(part, part, s.send.at[stage], s.recv.at[0, 0], me).wait_send()
            local(s.state, s.state, store_sem).wait()
        from_all(small_land, small_send, small_recv).wait_send()
        from_all(norm_land, norm_send, norm_recv).wait_send()
        from_all(tile_land, tile_send, tile_recv).wait_send()
        from_all(replica_small, rep_send, rep_recv).wait()
        local(small_wide, replica_small.at[me], copy_sem).wait()

    def pack_state(wide, vec):
        flat = jnp.concatenate([wide.reshape(-1), vec.reshape(-1), jnp.zeros((160,), jnp.float32)])
        return flat.reshape(TILE)

    def local_step(*banks):
        grad_attn, grad_mlp, grad_wide, grad_vec = banks[0:4]
        states = [banks[4:8], banks[8:12], banks[12:16]]
        wide = grad_wide.reshape(4, 32, 64).transpose(1, 0, 2).reshape(32, 256)
        vec = grad_vec.reshape(38, 32, 16).transpose(1, 0, 2).reshape(32, 608)
        grad_small = jnp.concatenate([wide, vec, jnp.zeros((32, 160), jnp.bfloat16)], axis=1).reshape(32, 8, LANES)
        state_small = jnp.stack([pack_state(state[2], state[3]) for state in states])
        anywhere = pl.BlockSpec(memory_space=pl.ANY)
        vmem = pl.BlockSpec(memory_space=pltpu.VMEM)
        shape = jax.ShapeDtypeStruct
        scratch = []
        for spec in STREAMS:
            scratch += Stream(*spec).scratch()
        scratch += [
            pltpu.VMEM((32, 8, LANES), jnp.bfloat16),
            pltpu.VMEM((1, 8, LANES), jnp.float32),
            pltpu.VMEM(TILE, jnp.bfloat16),
            pltpu.VMEM((1, LANES), jnp.float32),
            pltpu.VMEM((32, 1, LANES), jnp.float32),
            pltpu.VMEM(TILE, jnp.float32),
            pltpu.VMEM((32, 8, LANES), jnp.float32),
            pltpu.VMEM(TILE, jnp.float32),
            pltpu.VMEM((2, 16, LANES), jnp.float32),
            pltpu.VMEM((2, 8, LANES), jnp.float32),
        ] + [pltpu.SemaphoreType.DMA] * 11
        outs = pl.pallas_call(
            kernel,
            name="lamb",
            out_shape=[
                shape((16, 262144), jnp.bfloat16), shape((8, 1048576), jnp.bfloat16), shape((32, 8, LANES), jnp.bfloat16),
                shape((16, 8192), jnp.float32), shape((16, 8192), jnp.float32), shape((16, 8192), jnp.float32),
                shape((8, 32768), jnp.float32), shape((8, 32768), jnp.float32), shape((8, 32768), jnp.float32),
                shape((3, 8, LANES), jnp.float32),
            ],
            in_specs=[anywhere, anywhere, vmem] + [anywhere] * 6 + [vmem],
            out_specs=[anywhere] * 9 + [vmem],
            scratch_shapes=scratch,
            compiler_params=pltpu.CompilerParams(has_side_effects=True, vmem_limit_bytes=62 * 2 ** 20),
        )(grad_attn, grad_mlp, grad_small, states[0][0], states[1][0], states[2][0], states[0][1], states[1][1], states[2][1], state_small)
        replica_small = outs[2].reshape(32, 1024)
        replica_wide = replica_small[:, 0:256].reshape(32, 4, 64).transpose(1, 0, 2).reshape(4, 2048)
        replica_vec = replica_small[:, 256:864].reshape(32, 38, 16).transpose(1, 0, 2).reshape(38, 512)
        new_small = outs[9].reshape(3, 1024)
        results = [outs[0], outs[1], replica_wide, replica_vec]
        for which in range(3):
            results += [outs[3 + which], outs[6 + which], new_small[which, 0:256].reshape(4, 64), new_small[which, 256:864].reshape(38, 16)]
        return tuple(results)

    return jax.shard_map(local_step, mesh=mesh, in_specs=(grad_spec,) * 4 + (shard_spec,) * 12, out_specs=(full_spec,) * 4 + (shard_spec,) * 12, check_vma=False)
```

```python
import jax
import jax.numpy as jnp
from jax import lax
from jax.sharding import PartitionSpec as P
from jax.experimental import pallas as pl
from jax.experimental.pallas import tpu as pltpu

STEP_NUMBER = 10
LEARN_RATE = 0.04
BETA_FIRST = 0.9
BETA_SECOND = 0.999
EPSILON = 1e-6
WEIGHT_DECAY = 0.01
MAX_NORM = 1.0

CHUNKS = 16
AHEAD = 2
SLOTS = AHEAD + 1
SCRATCHES = 14
DEVICES, HALF, OTHERS = 32, 16, 31
LANES = 128
VECTORS = 38
TILE = (8, 128)
CORE, X, Y, Z0, Z1 = 1, 2, 4, 8, 16
STREAMS = (
    ("mlp", 12288, 20480, (Y, X, Z0, Z1)),
    ("mlp", 0, 12288, (X, Y, Z0, Z1)),
    ("attn", 0, 8192, (Z0, X, Y, Z1)),
)
NATURAL = (Z1, Z0, Y, X, CORE)
ROWS = {"attn": 16, "mlp": 8}
SHARD = {"attn": 8192, "mlp": 32768}
MESH = pl.DeviceIdType.MESH
HIGHEST = lax.Precision.HIGHEST


def loop(first, stop, body):
    lax.fori_loop(first, stop, body, 0)


def direction(grad, weight, first, second, clip):
    clipped = clip * grad
    new_first = BETA_FIRST * first + (1.0 - BETA_FIRST) * clipped
    new_second = BETA_SECOND * second + (1.0 - BETA_SECOND) * (clipped * clipped)
    update = (new_first / (1.0 - BETA_FIRST ** STEP_NUMBER)) / (jnp.sqrt(new_second / (1.0 - BETA_SECOND ** STEP_NUMBER)) + EPSILON) + WEIGHT_DECAY * weight
    return update, new_first, new_second


def fold_lanes(value):
    total = value[:, 0:LANES]
    for column in range(LANES, value.shape[1], LANES):
        total = total + value[:, column:column + LANES]
    return total


class Stream:
    def __init__(self, bank, first_column, columns, order):
        self.bank, self.first_column, self.columns, self.order = bank, first_column, columns, order
        self.reduce_order = (order[0], CORE) + order[1:]
        self.rows = ROWS[bank]
        self.width = columns // CHUNKS
        self.tiles = self.rows // 8
        self.kept_dims = [weight for weight in NATURAL if weight != order[0]]

    def scratch(self):
        rows, width = self.rows, self.width
        return [
            pltpu.VMEM((SLOTS, self.tiles, 2, 2, 2, 2, 8, width), jnp.bfloat16),
            pltpu.VMEM((2, 16, rows, width), jnp.float32),
            pltpu.VMEM((CHUNKS, 8, rows, width), jnp.float32),
            pltpu.VMEM((CHUNKS, 4, rows, width), jnp.float32),
            pltpu.VMEM((CHUNKS, 2, rows, width), jnp.float32),
            pltpu.VMEM((CHUNKS, 1, rows, width), jnp.float32),
            pltpu.SemaphoreType.DMA((SLOTS,)),
            pltpu.SemaphoreType.DMA((2,)),
            pltpu.SemaphoreType.DMA((5, CHUNKS)),
            pltpu.SemaphoreType.DMA((5,)),
            pltpu.SemaphoreType.DMA((4, CHUNKS)),
            pltpu.SemaphoreType.DMA((4,)),
            pltpu.SemaphoreType.DMA,
            pltpu.SemaphoreType.DMA,
        ]

    def bind(self, refs, replica, state):
        self.replica, self.state = replica, state
        (self.own, self.acc, self.part8, self.part4, self.part2, self.part1,
         self.own_sem, self.core_send, self.recv, self.send, self.gather_recv, self.gather_sent, self.core_sent, self.core_got) = refs


def solution(mesh):
    grad_spec = P("data", None, None)
    shard_spec = P(None, "data")
    full_spec = P(None, None)

    def kernel(*refs):
        grads = {"attn": refs[0], "mlp": refs[1]}
        grad_wide, grad_vec = refs[2:4]
        given_states = {"attn": refs[4:7], "mlp": refs[7:10]}
        given_wide, given_vec = refs[10:13], refs[13:16]
        replicas = {"attn": refs[16], "mlp": refs[17]}
        replica_wide, replica_vec = refs[18:20]
        states = {"attn": refs[20], "mlp": refs[21]}
        state_wide, state_vec = refs[22:24]
        rest = refs[24:]
        streams = []
        for index, spec in enumerate(STREAMS):
            stream = Stream(*spec)
            stream.bind(rest[SCRATCHES * index:SCRATCHES * (index + 1)], replicas[stream.bank], states[stream.bank])
            streams.append(stream)
        (square_pad, vec_rows, vec_land, wide_land, vec_sums, vec_pack, wide_pack, vec_out, wide_out, vec_got, wide_got, vec_grad,
         norm_out, norm_land, tile_out, tile_land, square, row_attn, row_mlp,
         vec_send, vec_recv, wide_send, wide_recv, norm_send, norm_recv, tile_send, tile_recv,
         vec_sent, vec_back, wide_sent, wide_back, load_sem) = rest[SCRATCHES * len(streams):]

        me = lax.axis_index("data")
        bit = {w: (me // w) % 2 for w in (CORE, X, Y, Z0, Z1)}
        peer = {w: me + w - 2 * w * bit[w] for w in bit}

        def blocks(s, whole, columns, fixed):
            picks = [fixed.get(weight, slice(None)) for weight in NATURAL]
            return whole.at[(slice(None), *picks, slice(None), columns)]

        def chunk(s, k):
            start = s.first_column + k * s.width
            return pl.ds(start if isinstance(k, int) else pl.multiple_of(start, LANES), s.width)

        def every(s):
            return pl.ds(s.first_column, s.columns)

        def remote(src, dst, send_sem, recv_sem, device):
            return pltpu.make_async_remote_copy(src_ref=src, dst_ref=dst, send_sem=send_sem, recv_sem=recv_sem, device_id=(device,), device_id_type=MESH)

        def local(src, dst, sem):
            return pltpu.make_async_copy(src, dst, sem)

        def start_raw(s, k):
            slot = k % SLOTS
            first = s.order[0]
            given, kept = [{first: value} for value in (1 - bit[first], bit[first])]
            remote(blocks(s, grads[s.bank], chunk(s, k), given), blocks(s, s.replica, chunk(s, k), given), s.send.at[0], s.recv.at[0, k], peer[first]).start()
            local(blocks(s, grads[s.bank], chunk(s, k), kept), s.own.at[slot], s.own_sem.at[slot]).start()

        def add_raw(s, k):
            slot = k % 2
            mine = k % SLOTS
            local(s.own.at[mine], s.own.at[mine], s.own_sem.at[mine]).wait()
            first = s.order[0]
            landed = blocks(s, s.replica, chunk(s, k), {first: bit[first]})
            remote(landed, landed, s.send.at[0], s.recv.at[0, k], peer[first]).wait_recv()

            @pl.when(k >= 2)
            def _():
                remote(s.acc.at[slot, pl.ds(8, 8)], s.part8.at[k], s.core_send.at[slot], s.recv.at[1, k], peer[CORE]).wait_send()

            def body(rel, carry):
                place = {}
                left = rel
                for weight in reversed(s.reduce_order[1:]):
                    place[weight] = (bit[weight] + left) % 2
                    left = left // 2
                kept = [place[weight] for weight in s.kept_dims]
                place[first] = bit[first]
                owner = [place[weight] for weight in NATURAL]
                for tile in range(s.tiles):
                    got = s.replica[(tile, *owner, slice(None), chunk(s, k))]
                    s.acc[slot, rel, 8 * tile:8 * tile + 8] = s.own[(mine, tile, *kept)].astype(jnp.float32) + got.astype(jnp.float32)
                return carry

            loop(8, 16, body)
            remote(s.acc.at[slot, pl.ds(8, 8)], s.part8.at[k], s.core_send.at[slot], s.recv.at[1, k], peer[CORE]).start()
            loop(0, 8, body)

        def add_core(s, k):
            slot = k % 2
            remote(s.acc.at[slot, pl.ds(8, 8)], s.part8.at[k], s.core_send.at[slot], s.recv.at[1, k], peer[CORE]).wait_recv()

            def body(rel, carry):
                s.part8[k, rel] = s.part8[k, rel] + s.acc[slot, rel]
                return carry

            loop(4, 8, body)
            remote(s.part8.at[k, pl.ds(4, 4)], s.part4.at[k], s.send.at[2], s.recv.at[2, k], peer[s.order[1]]).start()
            loop(0, 4, body)

        def add_step(s, k, stage):
            held, got = (s.part8, s.part4) if stage == 2 else (s.part4, s.part2)
            half = 4 if stage == 2 else 2
            nxt = s.part2 if stage == 2 else s.part1
            remote(held.at[k, pl.ds(half, half)], got.at[k], s.send.at[stage], s.recv.at[stage, k], peer[s.order[stage - 1]]).wait_recv()

            def body(rel, carry):
                got[k, rel] = got[k, rel] + held[k, rel]
                return carry

            quarter = half // 2
            loop(quarter, half, body)
            remote(got.at[k, pl.ds(quarter, quarter)], nxt.at[k], s.send.at[stage + 1], s.recv.at[stage + 1, k], peer[s.order[stage]]).start()
            loop(0, quarter, body)

        def add_last(s, k):
            remote(s.part2.at[k, pl.ds(1, 1)], s.part1.at[k], s.send.at[4], s.recv.at[4, k], peer[s.order[3]]).wait_recv()
            grad = (s.part1[k, 0] + s.part2[k, 0]) * (1.0 / 32.0)
            s.part1[k, 0] = grad
            part = fold_lanes(grad * grad)
            for row in range(0, s.rows, 8):
                square[...] += part[row:row + 8]

        def to_all(block_for, land, send_sem, recv_sem):
            def body(d, carry):
                other = (me + d) % DEVICES
                remote(block_for(other), land.at[me], send_sem, recv_sem, other).start()
                return carry

            loop(1, DEVICES, body)

        def from_all(land, send_sem, recv_sem):
            blocks = land.at[pl.ds(0, OTHERS)]
            return remote(blocks, blocks, send_sem, recv_sem, me)

        for k in range(AHEAD):
            for s in streams:
                start_raw(s, k)
        for bank in states:
            for which in range(3):
                local(given_states[bank][which], states[bank].at[which], load_sem).start()
        for which in range(3):
            local(given_wide[which], state_wide.at[which], load_sem).start()
            local(given_vec[which], state_vec.at[which], load_sem).start()

        def turned(z):
            return pl.ds(z * LANES, LANES)

        square_pad[...] = jnp.zeros_like(square_pad)
        for z in range(4):
            square_pad[0:VECTORS] = grad_vec[0, :, turned(z)].astype(jnp.float32)
            rows = square_pad[...].T.astype(jnp.bfloat16)
            for place in range(8):
                vec_rows[8 * z + place] = rows[16 * place:16 * place + 16]

        def wide_tile(owner):
            return pl.ds(pl.multiple_of(owner // 2 * LANES, LANES), LANES)

        vec_land[me] = vec_rows[me]
        wide_land[me] = grad_wide[0, :, wide_tile(me)]
        to_all(lambda other: vec_rows.at[other], vec_land, vec_send, vec_recv)
        to_all(lambda other: grad_wide.at[0, :, wide_tile(other)], wide_land, wide_send, wide_recv)
        square[...] = jnp.zeros_like(square)

        stages = (add_raw, add_core, lambda s, k: add_step(s, k, 2), lambda s, k: add_step(s, k, 3), add_last)

        def reduce_step(t, carry):
            @pl.when(t + AHEAD < CHUNKS)
            def _():
                for s in streams:
                    start_raw(s, t + AHEAD)

            for lag in reversed(range(len(stages))):
                @pl.when(jnp.logical_and(t >= lag, t < CHUNKS + lag))
                def _(lag=lag):
                    for s in streams:
                        stages[lag](s, t - lag)

            return carry

        loop(0, CHUNKS + len(stages) - 1, reduce_step)

        from_all(vec_land, vec_send, vec_recv).wait_recv()
        from_all(wide_land, wide_send, wide_recv).wait_recv()

        def sum_all(land):
            total = land[0].astype(jnp.float32)
            for d in range(1, DEVICES):
                total = total + land[d].astype(jnp.float32)
            return total

        vec_full = sum_all(vec_land) * (1.0 / 32.0)
        wide_full = sum_all(wide_land) * (1.0 / 32.0)
        wide_full = jnp.where(bit[CORE] == 0, wide_full, pltpu.roll(wide_full, 64, 1))
        lane_wide = lax.broadcasted_iota(jnp.int32, (4, LANES), 1)
        wide_full = jnp.where(lane_wide < 64, wide_full, 0.0)
        vec_grad[...] = vec_full
        wide_pack[...] = wide_full
        norm_out[...] = (jnp.sum(square[...], axis=0, keepdims=True) + jnp.sum(vec_full * vec_full, axis=0, keepdims=True)
                         + jnp.sum(wide_full * wide_full, axis=0, keepdims=True))
        norm_land[me] = norm_out[...]

        to_all(lambda other: norm_out, norm_land, norm_send, norm_recv)

        for state in (states["attn"], states["mlp"], state_wide, state_vec):
            local(state, state, load_sem).wait()
        row_attn[...] = jnp.zeros_like(row_attn)
        row_mlp[...] = jnp.zeros_like(row_mlp)
        rows_of = {"attn": row_attn, "mlp": row_mlp}
        for s in streams:
            def weight_rows(k, carry, s=s):
                weight = s.state[0, :, chunk(s, k)]
                rows_of[s.bank][1] += fold_lanes(weight * weight)
                return carry
            loop(0, CHUNKS, weight_rows)

        from_all(norm_land, norm_send, norm_recv).wait_recv()
        total = jnp.zeros((1, LANES), jnp.float32)
        for d in range(DEVICES):
            total = total + norm_land[d]
        clip = jnp.minimum(1.0, MAX_NORM / jnp.sqrt(jnp.sum(total, axis=1, keepdims=True)))

        for s in streams:
            def move(k, carry, s=s):
                here = chunk(s, k)
                update, new_first, new_second = direction(s.part1[k, 0], *[s.state[which, :, here] for which in range(3)], clip)
                s.part1[k, 0] = update
                s.state[1, :, here] = new_first
                s.state[2, :, here] = new_second
                rows_of[s.bank][0] += fold_lanes(update * update)
                return carry
            loop(0, CHUNKS, move)
        vec_weight, wide_weight = state_vec[0], state_wide[0]
        vec_update, state_vec[1], state_vec[2] = direction(vec_grad[:, 0:VECTORS], vec_weight, state_vec[1], state_vec[2], clip)
        wide_update, state_wide[1], state_wide[2] = direction(wide_pack[:, 0:64], wide_weight, state_wide[1], state_wide[2], clip)
        vec_pack[...] = jnp.zeros_like(vec_pack)
        for which, value in enumerate((vec_update, vec_weight)):
            vec_pack[0:1, 0:VECTORS] = jnp.sum(value * value, axis=0, keepdims=True)
            vec_sums[which] = pltpu.roll(vec_pack[0:8], 64, 1)

        lane = lax.broadcasted_iota(jnp.int32, TILE, 1)
        row = lax.broadcasted_iota(jnp.int32, TILE, 0)
        tile = vec_sums[0] + pltpu.roll(vec_sums[1], 1, 0)
        wide_sums = [jnp.sum(value * value, axis=1, keepdims=True) for value in (wide_update, wide_weight)]
        wide_pack[...] = jnp.where(lane_wide == 3, wide_sums[0], 0.0) + jnp.where(lane_wide == 19, wide_sums[1], 0.0)
        tile_out[...] = tile
        tile_out[0:4] += wide_pack[...]
        tile = tile_out[...]
        for which, base in ((0, 0), (1, 16)):
            attn_sum = jnp.sum(row_attn[which], axis=1, keepdims=True)
            mlp_sum = jnp.sum(row_mlp[which], axis=1, keepdims=True)
            tile = tile + jnp.where(lane == base, attn_sum[0:8], 0.0) + jnp.where(lane == base + 1, attn_sum[8:16], 0.0) + jnp.where(lane == base + 2, mlp_sum, 0.0)
        tile_out[...] = tile
        tile_land[me] = tile

        to_all(lambda other: tile_out, tile_land, tile_send, tile_recv)

        from_all(tile_land, tile_send, tile_recv).wait_recv()
        sums = tile_land[0]
        for d in range(1, DEVICES):
            sums = sums + tile_land[d]

        def lane_column(index):
            return jnp.sum(jnp.where(lane == index, sums, 0.0), axis=1, keepdims=True)

        def scale(weight_square, update_square):
            return LEARN_RATE * (jnp.sqrt(weight_square) / jnp.sqrt(update_square))

        scale_attn = jnp.concatenate([scale(lane_column(16), lane_column(0)), scale(lane_column(17), lane_column(1))], axis=0)
        scales = {"attn": scale_attn, "mlp": scale(lane_column(18), lane_column(2))}

        turned_sums = pltpu.roll(jnp.where(row < 2, sums, 1.0), 64, 1)
        scale_vec = scale(turned_sums[1:2, 0:VECTORS], turned_sums[0:1, 0:VECTORS])
        vec_new = vec_weight - scale_vec * vec_update
        wide_new = wide_weight - scale(lane_column(19)[0:4], lane_column(3)[0:4]) * wide_update
        state_vec[0] = vec_new
        state_wide[0] = wide_new
        vec_pack[:, 0:VECTORS] = vec_new
        vec_out[...] = vec_pack[...].astype(jnp.bfloat16)
        wide_pack[...] = jnp.zeros_like(wide_pack)
        wide_pack[:, 0:64] = wide_new
        wide_out[...] = (wide_pack[...] + pltpu.roll(wide_pack[...], 64, 1)).astype(jnp.bfloat16)
        vec_got[me] = vec_out[...]
        wide_got[me] = wide_out[...]

        def gathered(s, columns, j, newest=None, core=0):
            fixed = {weight: bit[weight] for weight in s.order[:4 - j]}
            if newest is not None:
                weight = s.order[3 - newest]
                fixed[weight] = 1 - bit[weight]
            fixed[CORE] = (bit[CORE] + core) % 2
            return blocks(s, replicas[s.bank], columns, fixed)

        def gather_send(s, k, j):
            held = gathered(s, chunk(s, k), j)
            remote(held, held, s.gather_sent.at[j], s.gather_recv.at[j, k], peer[s.order[3 - j]]).start()

        def gather_wait(s, k, j):
            got = gathered(s, chunk(s, k), j, j)
            remote(got, got, s.gather_sent.at[j], s.gather_recv.at[j, k], me).wait_recv()

        def core_send(s, k, j):
            got = gathered(s, chunk(s, k), j, j)
            remote(got, got, s.core_sent, s.core_got, peer[CORE]).start()

        def renew(s, k):
            here = chunk(s, k)
            new_weight = s.state[0, :, here] - scales[s.bank] * s.part1[k, 0]
            s.state[0, :, here] = new_weight
            for tile in range(s.tiles):
                s.replica[(tile, *[bit[weight] for weight in NATURAL], slice(None), here)] = new_weight[8 * tile:8 * tile + 8].astype(jnp.bfloat16)

        def first_sends(s, k):
            mine = gathered(s, chunk(s, k), 0)
            gather_send(s, k, 0)
            remote(mine, mine, s.core_sent, s.core_got, peer[CORE]).start()

        def gather_step(t, carry):
            @pl.when(t < CHUNKS)
            def _():
                for s in streams:
                    renew(s, t)
                for s in streams:
                    first_sends(s, t)

            for j in (1, 2, 3):
                @pl.when(jnp.logical_and(t >= j, t < CHUNKS + j))
                def _(j=j):
                    for s in streams:
                        gather_wait(s, t - j, j - 1)
                        gather_send(s, t - j, j)
                        core_send(s, t - j, j - 1)

            @pl.when(t >= 4)
            def _():
                for s in streams:
                    gather_wait(s, t - 4, 3)
                    core_send(s, t - 4, 3)

            return carry

        gather_step(0, 0)
        to_all(lambda other: vec_out, vec_got, vec_sent, vec_back)
        to_all(lambda other: wide_out, wide_got, wide_sent, wide_back)
        loop(1, CHUNKS + 4, gather_step)

        from_all(vec_got, vec_sent, vec_back).wait()
        from_all(wide_got, wide_sent, wide_back).wait()
        for z in range(4):
            for place in range(8):
                square_pad[16 * place:16 * place + 16] = vec_got[8 * z + place].astype(jnp.float32)
            replica_vec[:, turned(z)] = square_pad[...].T[0:VECTORS].astype(jnp.bfloat16)
        for pair in range(HALF):
            low, high = wide_got[2 * pair].astype(jnp.float32), wide_got[2 * pair + 1].astype(jnp.float32)
            replica_wide[:, turned(pair)] = jnp.where(lane_wide < 64, low, high).astype(jnp.bfloat16)

        for s in streams:
            half = gathered(s, every(s), 4)
            remote(half, half, s.core_sent, s.core_got, me).wait()
            for j in range(4):
                held = gathered(s, every(s), j)
                remote(held, held, s.gather_sent.at[j], s.core_got, me).wait_send()
            first = s.order[0]
            landed = blocks(s, s.replica, every(s), {first: bit[first]})
            remote(landed, landed, s.send.at[0], s.recv.at[0, 0], me).wait_send()
            for last in (CHUNKS - 2, CHUNKS - 1):
                slot = last % 2
                remote(s.acc.at[slot, pl.ds(8, 8)], s.part8.at[last], s.core_send.at[slot], s.recv.at[1, last], me).wait_send()
            for stage, part in ((2, s.part4), (3, s.part2), (4, s.part1)):
                remote(part, part, s.send.at[stage], s.recv.at[0, 0], me).wait_send()
        from_all(vec_land, vec_send, vec_recv).wait_send()
        from_all(wide_land, wide_send, wide_recv).wait_send()
        from_all(norm_land, norm_send, norm_recv).wait_send()
        from_all(tile_land, tile_send, tile_recv).wait_send()

    def store(*refs):
        results, outs, sem = refs[:8], refs[8:24], refs[24]
        copies = []
        for index in range(4):
            copies.append((results[index], outs[index]))
            for which in range(3):
                copies.append((results[4 + index].at[which], outs[4 + 4 * which + index]))
        copies = [pltpu.make_async_copy(source, target, sem.at[index]) for index, (source, target) in enumerate(copies)]
        for copy in copies:
            copy.start()
        for copy in copies:
            copy.wait()

    def local_step(*banks):
        grad_attn, grad_mlp, grad_wide, grad_vec = banks[0:4]
        given = [[banks[4 + 4 * which + index] for which in range(3)] for index in range(4)]
        given[3] = [state.T for state in given[3]]
        bits = (2,) * 5
        grad_attn = grad_attn.reshape(2, 8, 32, 8192).transpose(0, 2, 1, 3).reshape(2, *bits, 8, 8192)
        grad_mlp = grad_mlp.reshape(8, 32, 32768).transpose(1, 0, 2).reshape(1, *bits, 8, 32768)
        anywhere = pl.BlockSpec(memory_space=pl.ANY)
        vmem = pl.BlockSpec(memory_space=pltpu.VMEM)
        narrow, wide = jnp.bfloat16, jnp.float32
        scratch = []
        for spec in STREAMS:
            scratch += Stream(*spec).scratch()
        small = [
            ((LANES, LANES), wide), ((DEVICES, HALF, LANES), narrow), ((DEVICES, HALF, LANES), narrow), ((DEVICES, 4, LANES), narrow),
            ((2, *TILE), wide), ((HALF, LANES), wide), ((4, LANES), wide), ((HALF, LANES), narrow), ((4, LANES), narrow),
            ((DEVICES, HALF, LANES), narrow), ((DEVICES, 4, LANES), narrow), ((HALF, LANES), wide),
            ((1, LANES), wide), ((DEVICES, 1, LANES), wide), (TILE, wide), ((DEVICES, *TILE), wide), (TILE, wide),
            ((2, HALF, LANES), wide), ((2, *TILE), wide),
        ]
        scratch += [pltpu.VMEM(*spec) for spec in small] + [pltpu.SemaphoreType.DMA] * 13
        replicas = [(grad_attn.shape, narrow), (grad_mlp.shape, narrow), (grad_wide.shape[1:], narrow), (grad_vec.shape[1:], narrow)]
        states = [((3, *state[0].shape), wide) for state in given]
        results = pl.pallas_call(
            kernel,
            name="lamb",
            out_shape=[pltpu.VMEM(*spec) for spec in replicas + states],
            in_specs=[anywhere, anywhere, vmem, vmem] + [anywhere] * 12,
            out_specs=[vmem] * 8,
            scratch_shapes=scratch,
            compiler_params=pltpu.CompilerParams(has_side_effects=True, vmem_limit_bytes=32 * 2 ** 20),
        )(grad_attn, grad_mlp, grad_wide, grad_vec, *[state for bank in given for state in bank])
        shape = jax.ShapeDtypeStruct
        outs = list(pl.pallas_call(
            store,
            name="store",
            out_shape=[shape(*spec) for spec in replicas] + [shape(spec[0][1:], wide) for spec in states] * 3,
            in_specs=[vmem] * 8,
            out_specs=[anywhere] * 16,
            scratch_shapes=[pltpu.SemaphoreType.DMA((16,))],
            compiler_params=pltpu.CompilerParams(vmem_limit_bytes=2 ** 20),
        )(*results))
        outs[0] = outs[0].reshape(2, 32, 8, 8192).transpose(0, 2, 1, 3).reshape(16, -1)
        outs[1] = outs[1].reshape(32, 8, 32768).transpose(1, 0, 2).reshape(8, -1)
        for index in (7, 11, 15):
            outs[index] = outs[index].T
        return tuple(outs)

    return jax.shard_map(local_step, mesh=mesh, in_specs=(grad_spec,) * 4 + (shard_spec,) * 12, out_specs=(full_spec,) * 4 + (shard_spec,) * 12, check_vma=False)
```

```python
import jax
import jax.numpy as jnp
from jax import lax
from jax.sharding import PartitionSpec as P
from jax.experimental import pallas as pl
from jax.experimental.pallas import tpu as pltpu

STEP_NUMBER = 10
LEARN_RATE = 0.04
BETA_FIRST = 0.9
BETA_SECOND = 0.999
EPSILON = 1e-6
WEIGHT_DECAY = 0.01
MAX_NORM = 1.0

AHEAD = 1
SLOTS = AHEAD + 1
SCRATCHES = 14
DEVICES, HALF, OTHERS = 32, 16, 31
LANES = 128
VECTORS = 38
TILE = (8, 128)
CORE, X, Y, Z0, Z1 = 1, 2, 4, 8, 16
ROUTES = (
    ("mlp", (Y, X, Z0, Z1), 12288),
    ("mlp", (X, Y, Z0, Z1), 0),
    ("attn", (Z0, X, Y, Z1), 0),
)
GROUPS = (
    (16, (10, 6, 4)),
)
NATURAL = (Z1, Z0, Y, X, CORE)
ROWS = {"attn": 16, "mlp": 8}
SHARD = {"attn": 8192, "mlp": 32768}
MESH = pl.DeviceIdType.MESH
HIGHEST = lax.Precision.HIGHEST


def loop(first, stop, body):
    lax.fori_loop(first, stop, body, 0)


def direction(grad, weight, first, second, clip):
    clipped = clip * grad
    new_first = BETA_FIRST * first + (1.0 - BETA_FIRST) * clipped
    new_second = BETA_SECOND * second + (1.0 - BETA_SECOND) * (clipped * clipped)
    update = (new_first / (1.0 - BETA_FIRST ** STEP_NUMBER)) / (jnp.sqrt(new_second / (1.0 - BETA_SECOND ** STEP_NUMBER)) + EPSILON) + WEIGHT_DECAY * weight
    return update, new_first, new_second


def fold_lanes(value):
    total = value[:, 0:LANES]
    for column in range(LANES, value.shape[1], LANES):
        total = total + value[:, column:column + LANES]
    return total


TOTAL = sum(chunks for chunks, _ in GROUPS)


class Stream:
    def __init__(self, bank, order, first_column, width, chunks, begin, gather_begin):
        self.bank, self.order, self.first_column, self.width, self.chunks = bank, order, first_column, width, chunks
        self.columns, self.begin, self.gather_begin = width * chunks, begin, gather_begin
        self.reduce_order = (order[0], CORE) + order[1:]
        self.rows = ROWS[bank]
        self.tiles = self.rows // 8
        self.kept_dims = [weight for weight in NATURAL if weight != order[0]]

    def scratch(self):
        rows, width = self.rows, self.width
        return [
            pltpu.VMEM((SLOTS, self.tiles, 2, 2, 2, 2, 8, width), jnp.bfloat16),
            pltpu.VMEM((2, 16, rows, width), jnp.float32),
            pltpu.VMEM((self.chunks, 8, rows, width), jnp.float32),
            pltpu.VMEM((self.chunks, 4, rows, width), jnp.float32),
            pltpu.VMEM((self.chunks, 2, rows, width), jnp.float32),
            pltpu.VMEM((self.chunks, 1, rows, width), jnp.float32),
            pltpu.SemaphoreType.DMA((SLOTS,)),
            pltpu.SemaphoreType.DMA((2,)),
            pltpu.SemaphoreType.DMA((5, self.chunks)),
            pltpu.SemaphoreType.DMA((5,)),
            pltpu.SemaphoreType.DMA((4, self.chunks)),
            pltpu.SemaphoreType.DMA((4,)),
            pltpu.SemaphoreType.DMA,
            pltpu.SemaphoreType.DMA,
        ]

    def bind(self, refs, replica, state):
        self.replica, self.state = replica, state
        (self.own, self.acc, self.part8, self.part4, self.part2, self.part1,
         self.own_sem, self.core_send, self.recv, self.send, self.gather_recv, self.gather_sent, self.core_sent, self.core_got) = refs


def make_streams():
    streams, begin = [], 0
    firsts = [route[2] for route in ROUTES]
    for chunks, tiles in GROUPS:
        for index, (bank, order, _) in enumerate(ROUTES):
            width = tiles[index] * LANES
            streams.append(Stream(bank, order, firsts[index], width, chunks, begin, TOTAL - begin - chunks))
            firsts[index] += width * chunks
        begin += chunks
    return streams


def solution(mesh):
    grad_spec = P("data", None, None)
    shard_spec = P(None, "data")
    full_spec = P(None, None)

    def kernel(*refs):
        grads = {"attn": refs[0], "mlp": refs[1]}
        given_wide_grad, given_vec_grad = refs[2:4]
        given_states = {"attn": refs[4:7], "mlp": refs[7:10]}
        given_wide, given_vec = refs[10:13], refs[13:16]
        replicas = {"attn": refs[16], "mlp": refs[17]}
        replica_wide, replica_vec = refs[18:20]
        states = {"attn": refs[20], "mlp": refs[21]}
        state_wide, state_vec = refs[22:24]
        rest = refs[24:]
        streams = make_streams()
        for index, stream in enumerate(streams):
            stream.bind(rest[SCRATCHES * index:SCRATCHES * (index + 1)], replicas[stream.bank], states[stream.bank])
        (square_pad, vec_rows, vec_land, wide_land, vec_sums, vec_pack, wide_pack, vec_out, wide_out, vec_got, wide_got, vec_grad, grad_wide, grad_vec,
         norm_out, norm_land, tile_out, tile_land, square, row_attn, row_mlp,
         vec_send, vec_recv, wide_send, wide_recv, norm_send, norm_recv, tile_send, tile_recv,
         vec_sent, vec_back, wide_sent, wide_back, load_sem, grad_sem) = rest[SCRATCHES * len(streams):]

        me = lax.axis_index("data")
        bit = {w: (me // w) % 2 for w in (CORE, X, Y, Z0, Z1)}
        peer = {w: me + w - 2 * w * bit[w] for w in bit}

        def blocks(s, whole, columns, fixed):
            picks = [fixed.get(weight, slice(None)) for weight in NATURAL]
            return whole.at[(slice(None), *picks, slice(None), columns)]

        def chunk(s, k):
            start = s.first_column + k * s.width
            return pl.ds(start if isinstance(k, int) else pl.multiple_of(start, LANES), s.width)

        def every(s):
            return pl.ds(s.first_column, s.columns)

        def remote(src, dst, send_sem, recv_sem, device):
            return pltpu.make_async_remote_copy(src_ref=src, dst_ref=dst, send_sem=send_sem, recv_sem=recv_sem, device_id=(device,), device_id_type=MESH)

        def local(src, dst, sem):
            return pltpu.make_async_copy(src, dst, sem)

        def start_raw(s, k):
            slot = k % SLOTS
            first = s.order[0]
            given, kept = [{first: value} for value in (1 - bit[first], bit[first])]
            remote(blocks(s, grads[s.bank], chunk(s, k), given), blocks(s, s.replica, chunk(s, k), given), s.send.at[0], s.recv.at[0, k], peer[first]).start()
            local(blocks(s, grads[s.bank], chunk(s, k), kept), s.own.at[slot], s.own_sem.at[slot]).start()

        def add_raw(s, k):
            slot = k % 2
            mine = k % SLOTS
            local(s.own.at[mine], s.own.at[mine], s.own_sem.at[mine]).wait()
            first = s.order[0]
            landed = blocks(s, s.replica, chunk(s, k), {first: bit[first]})
            remote(landed, landed, s.send.at[0], s.recv.at[0, k], peer[first]).wait_recv()

            @pl.when(k >= 2)
            def _():
                remote(s.acc.at[slot, pl.ds(8, 8)], s.part8.at[k], s.core_send.at[slot], s.recv.at[1, k], peer[CORE]).wait_send()

            def add_block(high, low):
                place = {first: bit[first]}
                for bits, weights in ((high, (CORE, s.order[1])), (low, s.order[2:])):
                    for shift, weight in ((2, weights[0]), (1, weights[1])):
                        place[weight] = (bit[weight] + bits // shift) % 2
                kept = [place[weight] for weight in s.kept_dims]
                owner = [place[weight] for weight in NATURAL]
                for tile in range(s.tiles):
                    got = s.replica[(tile, *owner, slice(None), chunk(s, k))]
                    s.acc[slot, 4 * high + low, 8 * tile:8 * tile + 8] = s.own[(mine, tile, *kept)].astype(jnp.float32) + got.astype(jnp.float32)

            def body(high, carry):
                for low in range(4):
                    add_block(high, low)
                return carry

            loop(2, 4, body)
            remote(s.acc.at[slot, pl.ds(8, 8)], s.part8.at[k], s.core_send.at[slot], s.recv.at[1, k], peer[CORE]).start()
            loop(0, 2, body)

        def add_core(s, k):
            slot = k % 2
            remote(s.acc.at[slot, pl.ds(8, 8)], s.part8.at[k], s.core_send.at[slot], s.recv.at[1, k], peer[CORE]).wait_recv()

            def body(rel, carry):
                s.part8[k, rel] = s.part8[k, rel] + s.acc[slot, rel]
                return carry

            loop(4, 8, body)
            remote(s.part8.at[k, pl.ds(4, 4)], s.part4.at[k], s.send.at[2], s.recv.at[2, k], peer[s.order[1]]).start()
            loop(0, 4, body)

        def add_step(s, k, stage):
            held, got = (s.part8, s.part4) if stage == 2 else (s.part4, s.part2)
            half = 4 if stage == 2 else 2
            nxt = s.part2 if stage == 2 else s.part1
            remote(held.at[k, pl.ds(half, half)], got.at[k], s.send.at[stage], s.recv.at[stage, k], peer[s.order[stage - 1]]).wait_recv()

            def body(rel, carry):
                got[k, rel] = got[k, rel] + held[k, rel]
                return carry

            quarter = half // 2
            loop(quarter, half, body)
            remote(got.at[k, pl.ds(quarter, quarter)], nxt.at[k], s.send.at[stage + 1], s.recv.at[stage + 1, k], peer[s.order[stage]]).start()
            loop(0, quarter, body)

        def add_last(s, k):
            remote(s.part2.at[k, pl.ds(1, 1)], s.part1.at[k], s.send.at[4], s.recv.at[4, k], peer[s.order[3]]).wait_recv()
            grad = (s.part1[k, 0] + s.part2[k, 0]) * (1.0 / 32.0)
            s.part1[k, 0] = grad
            part = fold_lanes(grad * grad)
            for row in range(0, s.rows, 8):
                square[...] += part[row:row + 8]

        def at(chosen, time, begin, act):
            for first in sorted({getattr(s, begin) for s in chosen}):
                group = [s for s in chosen if getattr(s, begin) == first]
                k = time - first

                def run(group=group, k=k):
                    for s in group:
                        act(s, k)

                if isinstance(k, int):
                    if 0 <= k < group[0].chunks:
                        run()
                else:
                    pl.when(jnp.logical_and(k >= 0, k < group[0].chunks))(run)

        def to_all(block_for, land, send_sem, recv_sem):
            def body(d, carry):
                other = (me + d) % DEVICES
                remote(block_for(other), land.at[me], send_sem, recv_sem, other).start()
                return carry

            loop(1, DEVICES, body)

        def from_all(land, send_sem, recv_sem):
            blocks = land.at[pl.ds(0, OTHERS)]
            return remote(blocks, blocks, send_sem, recv_sem, me)

        barrier = pltpu.get_barrier_semaphore()
        for weight in NATURAL:
            pl.semaphore_signal(barrier, inc=1, device_id=(peer[weight],), device_id_type=MESH)
        pl.semaphore_wait(barrier, len(NATURAL))
        for t in range(AHEAD):
            at(streams, t, "begin", start_raw)
        local(given_wide_grad.at[0], grad_wide, grad_sem).start()
        local(given_vec_grad.at[0], grad_vec, grad_sem).start()
        for bank in states:
            for which in range(3):
                local(given_states[bank][which], states[bank].at[which], load_sem).start()
        for which in range(3):
            local(given_wide[which], state_wide.at[which], load_sem).start()
            local(given_vec[which], state_vec.at[which], load_sem).start()

        def turned(z):
            return pl.ds(z * LANES, LANES)

        local(grad_wide, grad_wide, grad_sem).wait()
        local(grad_vec, grad_vec, grad_sem).wait()
        square_pad[...] = jnp.zeros_like(square_pad)
        for z in range(4):
            square_pad[0:VECTORS] = grad_vec[:, turned(z)].astype(jnp.float32)
            rows = square_pad[...].T.astype(jnp.bfloat16)
            for place in range(8):
                vec_rows[8 * z + place] = rows[16 * place:16 * place + 16]

        def wide_tile(owner):
            return pl.ds(pl.multiple_of(owner // 2 * LANES, LANES), LANES)

        vec_land[me] = vec_rows[me]
        wide_land[me] = grad_wide[:, wide_tile(me)]
        def start_small():
            to_all(lambda other: vec_rows.at[other], vec_land, vec_send, vec_recv)
            to_all(lambda other: grad_wide.at[:, wide_tile(other)], wide_land, wide_send, wide_recv)

        square[...] = jnp.zeros_like(square)

        stages = (add_raw, add_core, lambda s, k: add_step(s, k, 2), lambda s, k: add_step(s, k, 3), add_last)

        def reduce_step(t, carry):
            at(streams, t + AHEAD, "begin", start_raw)
            for lag in reversed(range(len(stages))):
                at(streams, t - lag, "begin", stages[lag])
            return carry

        loop(0, TOTAL - 1, reduce_step)
        start_small()
        loop(TOTAL - 1, TOTAL + len(stages) - 1, reduce_step)

        from_all(vec_land, vec_send, vec_recv).wait_recv()
        from_all(wide_land, wide_send, wide_recv).wait_recv()

        def sum_all(land):
            total = land[0].astype(jnp.float32)
            for d in range(1, DEVICES):
                total = total + land[d].astype(jnp.float32)
            return total

        vec_full = sum_all(vec_land) * (1.0 / 32.0)
        wide_full = sum_all(wide_land) * (1.0 / 32.0)
        wide_full = jnp.where(bit[CORE] == 0, wide_full, pltpu.roll(wide_full, 64, 1))
        lane_wide = lax.broadcasted_iota(jnp.int32, (4, LANES), 1)
        wide_full = jnp.where(lane_wide < 64, wide_full, 0.0)
        vec_grad[...] = vec_full
        wide_pack[...] = wide_full
        norm_out[...] = (jnp.sum(square[...], axis=0, keepdims=True) + jnp.sum(vec_full * vec_full, axis=0, keepdims=True)
                         + jnp.sum(wide_full * wide_full, axis=0, keepdims=True))
        norm_land[me] = norm_out[...]

        to_all(lambda other: norm_out, norm_land, norm_send, norm_recv)

        for state in (states["attn"], states["mlp"], state_wide, state_vec):
            local(state, state, load_sem).wait()
        row_attn[...] = jnp.zeros_like(row_attn)
        row_mlp[...] = jnp.zeros_like(row_mlp)
        rows_of = {"attn": row_attn, "mlp": row_mlp}
        for s in streams:
            def weight_rows(k, carry, s=s):
                weight = s.state[0, :, chunk(s, k)]
                rows_of[s.bank][1] += fold_lanes(weight * weight)
                return carry
            loop(0, s.chunks, weight_rows)

        from_all(norm_land, norm_send, norm_recv).wait_recv()
        total = jnp.zeros((1, LANES), jnp.float32)
        for d in range(DEVICES):
            total = total + norm_land[d]
        clip = jnp.minimum(1.0, MAX_NORM / jnp.sqrt(jnp.sum(total, axis=1, keepdims=True)))

        for s in streams:
            def move(k, carry, s=s):
                here = chunk(s, k)
                update, new_first, new_second = direction(s.part1[k, 0], *[s.state[which, :, here] for which in range(3)], clip)
                s.part1[k, 0] = update
                s.state[1, :, here] = new_first
                s.state[2, :, here] = new_second
                rows_of[s.bank][0] += fold_lanes(update * update)
                return carry
            loop(0, s.chunks, move)
        vec_weight, wide_weight = state_vec[0], state_wide[0]
        vec_update, state_vec[1], state_vec[2] = direction(vec_grad[:, 0:VECTORS], vec_weight, state_vec[1], state_vec[2], clip)
        wide_update, state_wide[1], state_wide[2] = direction(wide_pack[:, 0:64], wide_weight, state_wide[1], state_wide[2], clip)
        vec_pack[...] = jnp.zeros_like(vec_pack)
        for which, value in enumerate((vec_update, vec_weight)):
            vec_pack[0:1, 0:VECTORS] = jnp.sum(value * value, axis=0, keepdims=True)
            vec_sums[which] = pltpu.roll(vec_pack[0:8], 64, 1)

        lane = lax.broadcasted_iota(jnp.int32, TILE, 1)
        row = lax.broadcasted_iota(jnp.int32, TILE, 0)
        tile = vec_sums[0] + pltpu.roll(vec_sums[1], 1, 0)
        wide_sums = [jnp.sum(value * value, axis=1, keepdims=True) for value in (wide_update, wide_weight)]
        wide_pack[...] = jnp.where(lane_wide == 3, wide_sums[0], 0.0) + jnp.where(lane_wide == 19, wide_sums[1], 0.0)
        tile_out[...] = tile
        tile_out[0:4] += wide_pack[...]
        tile = tile_out[...]
        for which, base in ((0, 0), (1, 16)):
            attn_sum = jnp.sum(row_attn[which], axis=1, keepdims=True)
            mlp_sum = jnp.sum(row_mlp[which], axis=1, keepdims=True)
            tile = tile + jnp.where(lane == base, attn_sum[0:8], 0.0) + jnp.where(lane == base + 1, attn_sum[8:16], 0.0) + jnp.where(lane == base + 2, mlp_sum, 0.0)
        tile_out[...] = tile
        tile_land[me] = tile

        to_all(lambda other: tile_out, tile_land, tile_send, tile_recv)

        from_all(tile_land, tile_send, tile_recv).wait_recv()
        sums = tile_land[0]
        for d in range(1, DEVICES):
            sums = sums + tile_land[d]

        def lane_column(index):
            return jnp.sum(jnp.where(lane == index, sums, 0.0), axis=1, keepdims=True)

        def scale(weight_square, update_square):
            return LEARN_RATE * (jnp.sqrt(weight_square) / jnp.sqrt(update_square))

        scale_attn = jnp.concatenate([scale(lane_column(16), lane_column(0)), scale(lane_column(17), lane_column(1))], axis=0)
        scales = {"attn": scale_attn, "mlp": scale(lane_column(18), lane_column(2))}

        turned_sums = pltpu.roll(jnp.where(row < 2, sums, 1.0), 64, 1)
        scale_vec = scale(turned_sums[1:2, 0:VECTORS], turned_sums[0:1, 0:VECTORS])
        vec_new = vec_weight - scale_vec * vec_update
        wide_new = wide_weight - scale(lane_column(19)[0:4], lane_column(3)[0:4]) * wide_update
        state_vec[0] = vec_new
        state_wide[0] = wide_new
        vec_pack[:, 0:VECTORS] = vec_new
        vec_out[...] = vec_pack[...].astype(jnp.bfloat16)
        wide_pack[...] = jnp.zeros_like(wide_pack)
        wide_pack[:, 0:64] = wide_new
        wide_out[...] = (wide_pack[...] + pltpu.roll(wide_pack[...], 64, 1)).astype(jnp.bfloat16)
        vec_got[me] = vec_out[...]
        wide_got[me] = wide_out[...]

        def gathered(s, columns, j, newest=None, core=0):
            fixed = {weight: bit[weight] for weight in s.order[:4 - j]}
            if newest is not None:
                weight = s.order[3 - newest]
                fixed[weight] = 1 - bit[weight]
            fixed[CORE] = (bit[CORE] + core) % 2
            return blocks(s, replicas[s.bank], columns, fixed)

        def gather_send(s, k, j):
            held = gathered(s, chunk(s, k), j)
            remote(held, held, s.gather_sent.at[j], s.gather_recv.at[j, k], peer[s.order[3 - j]]).start()

        def gather_wait(s, k, j):
            got = gathered(s, chunk(s, k), j, j)
            remote(got, got, s.gather_sent.at[j], s.gather_recv.at[j, k], me).wait_recv()

        def core_send(s, k, j):
            got = gathered(s, chunk(s, k), j, j)
            remote(got, got, s.core_sent, s.core_got, peer[CORE]).start()

        def renew(s, k):
            here = chunk(s, k)
            new_weight = s.state[0, :, here] - scales[s.bank] * s.part1[k, 0]
            s.state[0, :, here] = new_weight
            for tile in range(s.tiles):
                s.replica[(tile, *[bit[weight] for weight in NATURAL], slice(None), here)] = new_weight[8 * tile:8 * tile + 8].astype(jnp.bfloat16)

        def first_sends(s, k):
            mine = gathered(s, chunk(s, k), 0)
            gather_send(s, k, 0)
            remote(mine, mine, s.core_sent, s.core_got, peer[CORE]).start()

        def gather_last(s, k):
            gather_wait(s, k, 3)
            core_send(s, k, 3)

        def gather_next(s, k, j):
            gather_wait(s, k, j - 1)
            gather_send(s, k, j)
            core_send(s, k, j - 1)

        def gather_step(t, carry):
            at(streams, t, "gather_begin", renew)
            at(streams, t, "gather_begin", first_sends)
            for j in (1, 2, 3):
                at(streams, t - j, "gather_begin", lambda s, k, j=j: gather_next(s, k, j))
            at(streams, t - 4, "gather_begin", gather_last)
            return carry

        gather_step(0, 0)
        to_all(lambda other: vec_out, vec_got, vec_sent, vec_back)
        to_all(lambda other: wide_out, wide_got, wide_sent, wide_back)
        loop(1, TOTAL, gather_step)

        from_all(vec_got, vec_sent, vec_back).wait()
        from_all(wide_got, wide_sent, wide_back).wait()
        for z in range(4):
            for place in range(8):
                square_pad[16 * place:16 * place + 16] = vec_got[8 * z + place].astype(jnp.float32)
            replica_vec[:, turned(z)] = square_pad[...].T[0:VECTORS].astype(jnp.bfloat16)
        for pair in range(HALF):
            low, high = wide_got[2 * pair].astype(jnp.float32), wide_got[2 * pair + 1].astype(jnp.float32)
            replica_wide[:, turned(pair)] = jnp.where(lane_wide < 64, low, high).astype(jnp.bfloat16)

        loop(TOTAL, TOTAL + 4, gather_step)

        for s in streams:
            half = gathered(s, every(s), 4)
            remote(half, half, s.core_sent, s.core_got, me).wait()
            for j in range(4):
                held = gathered(s, every(s), j)
                remote(held, held, s.gather_sent.at[j], s.core_got, me).wait_send()
            first = s.order[0]
            landed = blocks(s, s.replica, every(s), {first: bit[first]})
            remote(landed, landed, s.send.at[0], s.recv.at[0, 0], me).wait_send()
            for last in range(s.chunks - 2, s.chunks):
                slot = last % 2
                remote(s.acc.at[slot, pl.ds(8, 8)], s.part8.at[last], s.core_send.at[slot], s.recv.at[1, last], me).wait_send()
            for stage, part in ((2, s.part4), (3, s.part2), (4, s.part1)):
                remote(part, part, s.send.at[stage], s.recv.at[0, 0], me).wait_send()
        from_all(vec_land, vec_send, vec_recv).wait_send()
        from_all(wide_land, wide_send, wide_recv).wait_send()
        from_all(norm_land, norm_send, norm_recv).wait_send()
        from_all(tile_land, tile_send, tile_recv).wait_send()

    def store(*refs):
        results, outs, sem = refs[:8], refs[8:24], refs[24]
        copies = []
        for index in range(4):
            copies.append((results[index], outs[index]))
            for which in range(3):
                copies.append((results[4 + index].at[which], outs[4 + 4 * which + index]))
        copies = [pltpu.make_async_copy(source, target, sem.at[index]) for index, (source, target) in enumerate(copies)]
        for copy in copies:
            copy.start()
        for copy in copies:
            copy.wait()

    def local_step(*banks):
        grad_attn, grad_mlp, grad_wide, grad_vec = banks[0:4]
        given = [[banks[4 + 4 * which + index] for which in range(3)] for index in range(4)]
        given[3] = [state.T for state in given[3]]
        bits = (2,) * 5
        grad_attn = grad_attn.reshape(2, 8, 32, 8192).transpose(0, 2, 1, 3).reshape(2, *bits, 8, 8192)
        grad_mlp = grad_mlp.reshape(8, 32, 32768).transpose(1, 0, 2).reshape(1, *bits, 8, 32768)
        anywhere = pl.BlockSpec(memory_space=pl.ANY)
        vmem = pl.BlockSpec(memory_space=pltpu.VMEM)
        narrow, wide = jnp.bfloat16, jnp.float32
        scratch = []
        streams = make_streams()
        for stream in streams:
            scratch += stream.scratch()
        small = [
            ((LANES, LANES), wide), ((DEVICES, HALF, LANES), narrow), ((DEVICES, HALF, LANES), narrow), ((DEVICES, 4, LANES), narrow),
            ((2, *TILE), wide), ((HALF, LANES), wide), ((4, LANES), wide), ((HALF, LANES), narrow), ((4, LANES), narrow),
            ((DEVICES, HALF, LANES), narrow), ((DEVICES, 4, LANES), narrow), ((HALF, LANES), wide), (grad_wide.shape[1:], narrow), (grad_vec.shape[1:], narrow),
            ((1, LANES), wide), ((DEVICES, 1, LANES), wide), (TILE, wide), ((DEVICES, *TILE), wide), (TILE, wide),
            ((2, HALF, LANES), wide), ((2, *TILE), wide),
        ]
        scratch += [pltpu.VMEM(*spec) for spec in small] + [pltpu.SemaphoreType.DMA] * 14
        replicas = [(grad_attn.shape, narrow), (grad_mlp.shape, narrow), (grad_wide.shape[1:], narrow), (grad_vec.shape[1:], narrow)]
        states = [((3, *state[0].shape), wide) for state in given]
        results = pl.pallas_call(
            kernel,
            name="lamb",
            out_shape=[pltpu.VMEM(*spec) for spec in replicas + states],
            in_specs=[anywhere] * 16,
            out_specs=[vmem] * 8,
            scratch_shapes=scratch,
            compiler_params=pltpu.CompilerParams(has_side_effects=True, collective_id=0, vmem_limit_bytes=32 * 2 ** 20),
        )(grad_attn, grad_mlp, grad_wide, grad_vec, *[state for bank in given for state in bank])
        shape = jax.ShapeDtypeStruct
        outs = list(pl.pallas_call(
            store,
            name="store",
            out_shape=[shape(*spec) for spec in replicas] + [shape(spec[0][1:], wide) for spec in states] * 3,
            in_specs=[vmem] * 8,
            out_specs=[anywhere] * 16,
            scratch_shapes=[pltpu.SemaphoreType.DMA((16,))],
            compiler_params=pltpu.CompilerParams(vmem_limit_bytes=2 ** 20),
        )(*results))
        outs[0] = outs[0].reshape(2, 32, 8, 8192).transpose(0, 2, 1, 3).reshape(16, -1)
        outs[1] = outs[1].reshape(32, 8, 32768).transpose(1, 0, 2).reshape(8, -1)
        for index in (7, 11, 15):
            outs[index] = outs[index].T
        return tuple(outs)

    return jax.shard_map(local_step, mesh=mesh, in_specs=(grad_spec,) * 4 + (shard_spec,) * 12, out_specs=(full_spec,) * 4 + (shard_spec,) * 12, check_vma=False)
```

```python
import jax
import jax.numpy as jnp
from jax import lax
from jax.sharding import PartitionSpec as P
from jax.experimental import pallas as pl
from jax.experimental.pallas import tpu as pltpu

STEP_NUMBER = 10
LEARN_RATE = 0.04
BETA_FIRST = 0.9
BETA_SECOND = 0.999
EPSILON = 1e-6
WEIGHT_DECAY = 0.01
MAX_NORM = 1.0

AHEAD = 1
SLOTS = AHEAD + 1
SCRATCHES = 14
DEVICES, HALF, OTHERS = 32, 16, 31
LANES = 128
VECTORS = 38
TILE = (8, 128)
CORE, X, Y, Z0, Z1 = 1, 2, 4, 8, 16
ROUTES = (
    ("mlp", (Y, X, Z0, Z1), 12288),
    ("mlp", (X, Y, Z0, Z1), 0),
    ("attn", (Z0, X, Y, Z1), 0),
)
GROUPS = (
    (16, (10, 6, 4)),
)
NATURAL = (Z1, Z0, Y, X, CORE)
ROWS = {"attn": 16, "mlp": 8}
SHARD = {"attn": 8192, "mlp": 32768}
MESH = pl.DeviceIdType.MESH
HIGHEST = lax.Precision.HIGHEST


def loop(first, stop, body):
    lax.fori_loop(first, stop, body, 0)


def direction(grad, weight, first, second, clip):
    clipped = clip * grad
    new_first = BETA_FIRST * first + (1.0 - BETA_FIRST) * clipped
    new_second = BETA_SECOND * second + (1.0 - BETA_SECOND) * (clipped * clipped)
    update = (new_first / (1.0 - BETA_FIRST ** STEP_NUMBER)) / (jnp.sqrt(new_second / (1.0 - BETA_SECOND ** STEP_NUMBER)) + EPSILON) + WEIGHT_DECAY * weight
    return update, new_first, new_second


def fold_lanes(value):
    total = value[:, 0:LANES]
    for column in range(LANES, value.shape[1], LANES):
        total = total + value[:, column:column + LANES]
    return total


TOTAL = sum(chunks for chunks, _ in GROUPS)


class Stream:
    def __init__(self, bank, order, first_column, width, chunks, begin, gather_begin):
        self.bank, self.order, self.first_column, self.width, self.chunks = bank, order, first_column, width, chunks
        self.columns, self.begin, self.gather_begin = width * chunks, begin, gather_begin
        self.reduce_order = (order[0], CORE) + order[1:]
        self.rows = ROWS[bank]
        self.tiles = self.rows // 8
        self.kept_dims = [weight for weight in NATURAL if weight != order[0]]

    def scratch(self):
        rows, width = self.rows, self.width
        return [
            pltpu.VMEM((SLOTS, self.tiles, 2, 2, 2, 2, 8, width), jnp.bfloat16),
            pltpu.VMEM((2, 16, rows, width), jnp.float32),
            pltpu.VMEM((self.chunks, 8, rows, width), jnp.float32),
            pltpu.VMEM((self.chunks, 4, rows, width), jnp.float32),
            pltpu.VMEM((self.chunks, 2, rows, width), jnp.float32),
            pltpu.VMEM((self.chunks, 1, rows, width), jnp.float32),
            pltpu.SemaphoreType.DMA((SLOTS,)),
            pltpu.SemaphoreType.DMA((2,)),
            pltpu.SemaphoreType.DMA((5, self.chunks)),
            pltpu.SemaphoreType.DMA((5,)),
            pltpu.SemaphoreType.DMA((4, self.chunks)),
            pltpu.SemaphoreType.DMA((4,)),
            pltpu.SemaphoreType.DMA,
            pltpu.SemaphoreType.DMA,
        ]

    def bind(self, refs, replica, state):
        self.replica, self.state = replica, state
        (self.own, self.acc, self.part8, self.part4, self.part2, self.part1,
         self.own_sem, self.core_send, self.recv, self.send, self.gather_recv, self.gather_sent, self.core_sent, self.core_got) = refs


def make_streams():
    streams, begin = [], 0
    firsts = [route[2] for route in ROUTES]
    for chunks, tiles in GROUPS:
        for index, (bank, order, _) in enumerate(ROUTES):
            width = tiles[index] * LANES
            streams.append(Stream(bank, order, firsts[index], width, chunks, begin, TOTAL - begin - chunks))
            firsts[index] += width * chunks
        begin += chunks
    return streams


def solution(mesh):
    grad_spec = P("data", None, None)
    shard_spec = P(None, "data")
    full_spec = P(None, None)

    def kernel(*refs):
        grads = {"attn": refs[0], "mlp": refs[1]}
        given_wide_grad, given_vec_grad = refs[2:4]
        given_states = {"attn": refs[4:7], "mlp": refs[7:10]}
        given_wide, given_vec = refs[10:13], refs[13:16]
        replicas = {"attn": refs[16], "mlp": refs[17]}
        replica_wide, replica_vec = refs[18:20]
        states = {"attn": refs[20], "mlp": refs[21]}
        state_wide, state_vec = refs[22:24]
        rest = refs[24:]
        streams = make_streams()
        for index, stream in enumerate(streams):
            stream.bind(rest[SCRATCHES * index:SCRATCHES * (index + 1)], replicas[stream.bank], states[stream.bank])
        (square_pad, vec_rows, vec_land, wide_land, vec_sums, vec_pack, wide_pack, vec_out, wide_out, vec_got, wide_got, vec_grad, grad_wide, grad_vec,
         norm_out, norm_land, tile_out, tile_land, square, row_attn, row_mlp,
         vec_send, vec_recv, wide_send, wide_recv, norm_send, norm_recv, tile_send, tile_recv,
         vec_sent, vec_back, wide_sent, wide_back, load_sem, grad_sem) = rest[SCRATCHES * len(streams):]

        me = lax.axis_index("data")
        bit = {w: (me // w) % 2 for w in (CORE, X, Y, Z0, Z1)}
        peer = {w: me + w - 2 * w * bit[w] for w in bit}

        def blocks(s, whole, columns, fixed):
            picks = [fixed.get(weight, slice(None)) for weight in NATURAL]
            return whole.at[(slice(None), *picks, slice(None), columns)]

        def chunk(s, k):
            start = s.first_column + k * s.width
            return pl.ds(start if isinstance(k, int) else pl.multiple_of(start, LANES), s.width)

        def every(s):
            return pl.ds(s.first_column, s.columns)

        def remote(src, dst, send_sem, recv_sem, device):
            return pltpu.make_async_remote_copy(src_ref=src, dst_ref=dst, send_sem=send_sem, recv_sem=recv_sem, device_id=(device,), device_id_type=MESH)

        def local(src, dst, sem):
            return pltpu.make_async_copy(src, dst, sem)

        def start_raw(s, k):
            slot = k % SLOTS
            first = s.order[0]
            given, kept = [{first: value} for value in (1 - bit[first], bit[first])]
            remote(blocks(s, grads[s.bank], chunk(s, k), given), blocks(s, s.replica, chunk(s, k), given), s.send.at[0], s.recv.at[0, k], peer[first]).start()
            local(blocks(s, grads[s.bank], chunk(s, k), kept), s.own.at[slot], s.own_sem.at[slot]).start()

        def add_raw(s, k):
            slot = k % 2
            mine = k % SLOTS
            local(s.own.at[mine], s.own.at[mine], s.own_sem.at[mine]).wait()
            first = s.order[0]
            landed = blocks(s, s.replica, chunk(s, k), {first: bit[first]})
            remote(landed, landed, s.send.at[0], s.recv.at[0, k], peer[first]).wait_recv()

            @pl.when(k >= 2)
            def _():
                remote(s.acc.at[slot, pl.ds(8, 8)], s.part8.at[k], s.core_send.at[slot], s.recv.at[1, k], peer[CORE]).wait_send()

            def add_block(high, low):
                place = {first: bit[first]}
                for bits, weights in ((high, (CORE, s.order[1])), (low, s.order[2:])):
                    for shift, weight in ((2, weights[0]), (1, weights[1])):
                        place[weight] = (bit[weight] + bits // shift) % 2
                kept = [place[weight] for weight in s.kept_dims]
                owner = [place[weight] for weight in NATURAL]
                for tile in range(s.tiles):
                    got = s.replica[(tile, *owner, slice(None), chunk(s, k))]
                    s.acc[slot, 4 * high + low, 8 * tile:8 * tile + 8] = s.own[(mine, tile, *kept)].astype(jnp.float32) + got.astype(jnp.float32)

            def body(high, carry):
                for low in range(4):
                    add_block(high, low)
                return carry

            loop(2, 4, body)
            remote(s.acc.at[slot, pl.ds(8, 8)], s.part8.at[k], s.core_send.at[slot], s.recv.at[1, k], peer[CORE]).start()
            loop(0, 2, body)

        def add_core(s, k):
            slot = k % 2
            remote(s.acc.at[slot, pl.ds(8, 8)], s.part8.at[k], s.core_send.at[slot], s.recv.at[1, k], peer[CORE]).wait_recv()

            def body(rel, carry):
                s.part8[k, rel] = s.part8[k, rel] + s.acc[slot, rel]
                return carry

            loop(4, 8, body)
            remote(s.part8.at[k, pl.ds(4, 4)], s.part4.at[k], s.send.at[2], s.recv.at[2, k], peer[s.order[1]]).start()
            loop(0, 4, body)

        def add_step(s, k, stage):
            held, got = (s.part8, s.part4) if stage == 2 else (s.part4, s.part2)
            half = 4 if stage == 2 else 2
            nxt = s.part2 if stage == 2 else s.part1
            remote(held.at[k, pl.ds(half, half)], got.at[k], s.send.at[stage], s.recv.at[stage, k], peer[s.order[stage - 1]]).wait_recv()

            def body(rel, carry):
                got[k, rel] = got[k, rel] + held[k, rel]
                return carry

            quarter = half // 2
            loop(quarter, half, body)
            remote(got.at[k, pl.ds(quarter, quarter)], nxt.at[k], s.send.at[stage + 1], s.recv.at[stage + 1, k], peer[s.order[stage]]).start()
            loop(0, quarter, body)

        def add_last(s, k):
            remote(s.part2.at[k, pl.ds(1, 1)], s.part1.at[k], s.send.at[4], s.recv.at[4, k], peer[s.order[3]]).wait_recv()
            grad = (s.part1[k, 0] + s.part2[k, 0]) * (1.0 / 32.0)
            s.part1[k, 0] = grad
            part = fold_lanes(grad * grad)
            for row in range(0, s.rows, 8):
                square[...] += part[row:row + 8]

        def at(chosen, time, begin, act):
            for first in sorted({getattr(s, begin) for s in chosen}):
                group = [s for s in chosen if getattr(s, begin) == first]
                k = time - first

                def run(group=group, k=k):
                    for s in group:
                        act(s, k)

                if isinstance(k, int):
                    if 0 <= k < group[0].chunks:
                        run()
                else:
                    pl.when(jnp.logical_and(k >= 0, k < group[0].chunks))(run)

        def to_all(block_for, land, send_sem, recv_sem):
            def body(d, carry):
                other = (me + d) % DEVICES
                remote(block_for(other), land.at[me], send_sem, recv_sem, other).start()
                return carry

            loop(1, DEVICES, body)

        def from_all(land, send_sem, recv_sem):
            blocks = land.at[pl.ds(0, OTHERS)]
            return remote(blocks, blocks, send_sem, recv_sem, me)

        barrier = pltpu.get_barrier_semaphore()
        for weight in NATURAL:
            pl.semaphore_signal(barrier, inc=1, device_id=(peer[weight],), device_id_type=MESH)
        pl.semaphore_wait(barrier, len(NATURAL))
        for t in range(AHEAD):
            at(streams, t, "begin", start_raw)
        local(given_wide_grad.at[0], grad_wide, grad_sem).start()
        local(given_vec_grad.at[0], grad_vec, grad_sem).start()
        for bank in states:
            for which in range(3):
                local(given_states[bank][which], states[bank].at[which], load_sem).start()
        for which in range(3):
            local(given_wide[which], state_wide.at[which], load_sem).start()
            local(given_vec[which], state_vec.at[which], load_sem).start()

        def turned(z):
            return pl.ds(z * LANES, LANES)

        local(grad_wide, grad_wide, grad_sem).wait()
        local(grad_vec, grad_vec, grad_sem).wait()
        square_pad[...] = jnp.zeros_like(square_pad)
        for z in range(4):
            square_pad[0:VECTORS] = grad_vec[:, turned(z)].astype(jnp.float32)
            rows = square_pad[...].T.astype(jnp.bfloat16)
            for place in range(8):
                vec_rows[8 * z + place] = rows[16 * place:16 * place + 16]

        def wide_tile(owner):
            return pl.ds(pl.multiple_of(owner // 2 * LANES, LANES), LANES)

        vec_land[me] = vec_rows[me]
        wide_land[me] = grad_wide[:, wide_tile(me)]
        def start_small():
            to_all(lambda other: vec_rows.at[other], vec_land, vec_send, vec_recv)
            to_all(lambda other: grad_wide.at[:, wide_tile(other)], wide_land, wide_send, wide_recv)

        square[...] = jnp.zeros_like(square)

        stages = (add_raw, add_core, lambda s, k: add_step(s, k, 2), lambda s, k: add_step(s, k, 3), add_last)

        def reduce_step(t, carry):
            at(streams, t + AHEAD, "begin", start_raw)
            for lag in range(len(stages)):
                at(streams, t - lag, "begin", stages[lag])
            return carry

        loop(0, TOTAL // 2, reduce_step)
        start_small()
        loop(TOTAL // 2, TOTAL, reduce_step)

        from_all(vec_land, vec_send, vec_recv).wait_recv()
        from_all(wide_land, wide_send, wide_recv).wait_recv()

        def sum_all(land):
            total = land[0].astype(jnp.float32)
            for d in range(1, DEVICES):
                total = total + land[d].astype(jnp.float32)
            return total

        vec_full = sum_all(vec_land) * (1.0 / 32.0)
        wide_full = sum_all(wide_land) * (1.0 / 32.0)
        wide_full = jnp.where(bit[CORE] == 0, wide_full, pltpu.roll(wide_full, 64, 1))
        lane_wide = lax.broadcasted_iota(jnp.int32, (4, LANES), 1)
        wide_full = jnp.where(lane_wide < 64, wide_full, 0.0)
        vec_grad[...] = vec_full
        wide_pack[...] = wide_full
        square[0:1] += jnp.sum(vec_full * vec_full, axis=0, keepdims=True) + jnp.sum(wide_full * wide_full, axis=0, keepdims=True)

        loop(TOTAL, TOTAL + len(stages) - 1, reduce_step)

        norm_out[...] = jnp.sum(square[...], axis=0, keepdims=True)
        norm_land[me] = norm_out[...]

        to_all(lambda other: norm_out, norm_land, norm_send, norm_recv)

        for state in (states["attn"], states["mlp"], state_wide, state_vec):
            local(state, state, load_sem).wait()
        row_attn[...] = jnp.zeros_like(row_attn)
        row_mlp[...] = jnp.zeros_like(row_mlp)
        rows_of = {"attn": row_attn, "mlp": row_mlp}
        for s in streams:
            def weight_rows(k, carry, s=s):
                weight = s.state[0, :, chunk(s, k)]
                rows_of[s.bank][1] += fold_lanes(weight * weight)
                return carry
            loop(0, s.chunks, weight_rows)

        from_all(norm_land, norm_send, norm_recv).wait_recv()
        total = jnp.zeros((1, LANES), jnp.float32)
        for d in range(DEVICES):
            total = total + norm_land[d]
        clip = jnp.minimum(1.0, MAX_NORM / jnp.sqrt(jnp.sum(total, axis=1, keepdims=True)))

        for s in streams:
            def move(k, carry, s=s):
                here = chunk(s, k)
                update, new_first, new_second = direction(s.part1[k, 0], *[s.state[which, :, here] for which in range(3)], clip)
                s.part1[k, 0] = update
                s.state[1, :, here] = new_first
                s.state[2, :, here] = new_second
                rows_of[s.bank][0] += fold_lanes(update * update)
                return carry
            loop(0, s.chunks, move)
        vec_weight, wide_weight = state_vec[0], state_wide[0]
        vec_update, state_vec[1], state_vec[2] = direction(vec_grad[:, 0:VECTORS], vec_weight, state_vec[1], state_vec[2], clip)
        wide_update, state_wide[1], state_wide[2] = direction(wide_pack[:, 0:64], wide_weight, state_wide[1], state_wide[2], clip)
        vec_pack[...] = jnp.zeros_like(vec_pack)
        for which, value in enumerate((vec_update, vec_weight)):
            vec_pack[0:1, 0:VECTORS] = jnp.sum(value * value, axis=0, keepdims=True)
            vec_sums[which] = pltpu.roll(vec_pack[0:8], 64, 1)

        lane = lax.broadcasted_iota(jnp.int32, TILE, 1)
        row = lax.broadcasted_iota(jnp.int32, TILE, 0)
        tile = vec_sums[0] + pltpu.roll(vec_sums[1], 1, 0)
        wide_sums = [jnp.sum(value * value, axis=1, keepdims=True) for value in (wide_update, wide_weight)]
        wide_pack[...] = jnp.where(lane_wide == 3, wide_sums[0], 0.0) + jnp.where(lane_wide == 19, wide_sums[1], 0.0)
        tile_out[...] = tile
        tile_out[0:4] += wide_pack[...]
        tile = tile_out[...]
        for which, base in ((0, 0), (1, 16)):
            attn_sum = jnp.sum(row_attn[which], axis=1, keepdims=True)
            mlp_sum = jnp.sum(row_mlp[which], axis=1, keepdims=True)
            tile = tile + jnp.where(lane == base, attn_sum[0:8], 0.0) + jnp.where(lane == base + 1, attn_sum[8:16], 0.0) + jnp.where(lane == base + 2, mlp_sum, 0.0)
        tile_out[...] = tile
        tile_land[me] = tile

        to_all(lambda other: tile_out, tile_land, tile_send, tile_recv)

        from_all(tile_land, tile_send, tile_recv).wait_recv()
        sums = tile_land[0]
        for d in range(1, DEVICES):
            sums = sums + tile_land[d]

        def lane_column(index):
            return jnp.sum(jnp.where(lane == index, sums, 0.0), axis=1, keepdims=True)

        def scale(weight_square, update_square):
            return LEARN_RATE * (jnp.sqrt(weight_square) / jnp.sqrt(update_square))

        scale_attn = jnp.concatenate([scale(lane_column(16), lane_column(0)), scale(lane_column(17), lane_column(1))], axis=0)
        scales = {"attn": scale_attn, "mlp": scale(lane_column(18), lane_column(2))}

        def gathered(s, columns, j, newest=None, core=0):
            fixed = {weight: bit[weight] for weight in s.order[:4 - j]}
            if newest is not None:
                weight = s.order[3 - newest]
                fixed[weight] = 1 - bit[weight]
            fixed[CORE] = (bit[CORE] + core) % 2
            return blocks(s, replicas[s.bank], columns, fixed)

        def gather_send(s, k, j):
            held = gathered(s, chunk(s, k), j)
            remote(held, held, s.gather_sent.at[j], s.gather_recv.at[j, k], peer[s.order[3 - j]]).start()

        def gather_wait(s, k, j):
            got = gathered(s, chunk(s, k), j, j)
            remote(got, got, s.gather_sent.at[j], s.gather_recv.at[j, k], me).wait_recv()

        def core_send(s, k, j):
            got = gathered(s, chunk(s, k), j, j)
            remote(got, got, s.core_sent, s.core_got, peer[CORE]).start()

        def renew(s, k):
            here = chunk(s, k)
            new_weight = s.state[0, :, here] - scales[s.bank] * s.part1[k, 0]
            s.state[0, :, here] = new_weight
            for tile in range(s.tiles):
                s.replica[(tile, *[bit[weight] for weight in NATURAL], slice(None), here)] = new_weight[8 * tile:8 * tile + 8].astype(jnp.bfloat16)

        def first_sends(s, k):
            mine = gathered(s, chunk(s, k), 0)
            gather_send(s, k, 0)
            remote(mine, mine, s.core_sent, s.core_got, peer[CORE]).start()

        def gather_last(s, k):
            gather_wait(s, k, 3)
            core_send(s, k, 3)

        def gather_next(s, k, j):
            gather_wait(s, k, j - 1)
            gather_send(s, k, j)
            core_send(s, k, j - 1)

        def gather_step(t, carry):
            at(streams, t, "gather_begin", renew)
            at(streams, t, "gather_begin", first_sends)
            for j in (1, 2, 3):
                at(streams, t - j, "gather_begin", lambda s, k, j=j: gather_next(s, k, j))
            at(streams, t - 4, "gather_begin", gather_last)
            return carry

        loop(0, TOTAL // 2, gather_step)

        turned_sums = pltpu.roll(jnp.where(row < 2, sums, 1.0), 64, 1)
        scale_vec = scale(turned_sums[1:2, 0:VECTORS], turned_sums[0:1, 0:VECTORS])
        vec_new = vec_weight - scale_vec * vec_update
        wide_new = wide_weight - scale(lane_column(19)[0:4], lane_column(3)[0:4]) * wide_update
        state_vec[0] = vec_new
        state_wide[0] = wide_new
        vec_pack[:, 0:VECTORS] = vec_new
        vec_out[...] = vec_pack[...].astype(jnp.bfloat16)
        wide_pack[...] = jnp.zeros_like(wide_pack)
        wide_pack[:, 0:64] = wide_new
        wide_out[...] = (wide_pack[...] + pltpu.roll(wide_pack[...], 64, 1)).astype(jnp.bfloat16)
        vec_got[me] = vec_out[...]
        wide_got[me] = wide_out[...]
        to_all(lambda other: vec_out, vec_got, vec_sent, vec_back)
        to_all(lambda other: wide_out, wide_got, wide_sent, wide_back)
        loop(TOTAL // 2, TOTAL, gather_step)

        from_all(vec_got, vec_sent, vec_back).wait()
        from_all(wide_got, wide_sent, wide_back).wait()
        for z in range(4):
            for place in range(8):
                square_pad[16 * place:16 * place + 16] = vec_got[8 * z + place].astype(jnp.float32)
            replica_vec[:, turned(z)] = square_pad[...].T[0:VECTORS].astype(jnp.bfloat16)
        for pair in range(HALF):
            low, high = wide_got[2 * pair].astype(jnp.float32), wide_got[2 * pair + 1].astype(jnp.float32)
            replica_wide[:, turned(pair)] = jnp.where(lane_wide < 64, low, high).astype(jnp.bfloat16)

        loop(TOTAL, TOTAL + 4, gather_step)

        for s in streams:
            half = gathered(s, every(s), 4)
            remote(half, half, s.core_sent, s.core_got, me).wait()
            for j in range(4):
                held = gathered(s, every(s), j)
                remote(held, held, s.gather_sent.at[j], s.core_got, me).wait_send()
            first = s.order[0]
            landed = blocks(s, s.replica, every(s), {first: bit[first]})
            remote(landed, landed, s.send.at[0], s.recv.at[0, 0], me).wait_send()
            for last in range(s.chunks - 2, s.chunks):
                slot = last % 2
                remote(s.acc.at[slot, pl.ds(8, 8)], s.part8.at[last], s.core_send.at[slot], s.recv.at[1, last], me).wait_send()
            for stage, part in ((2, s.part4), (3, s.part2), (4, s.part1)):
                remote(part, part, s.send.at[stage], s.recv.at[0, 0], me).wait_send()
        from_all(vec_land, vec_send, vec_recv).wait_send()
        from_all(wide_land, wide_send, wide_recv).wait_send()
        from_all(norm_land, norm_send, norm_recv).wait_send()
        from_all(tile_land, tile_send, tile_recv).wait_send()

    def store(*refs):
        results, outs, sem = refs[:8], refs[8:24], refs[24]
        copies = []
        for index in range(4):
            parts = [(z1, z0) for z1 in range(2) for z0 in range(2)] if index < 2 else [None]
            for part in parts:
                pick = (slice(None), *part) if part else slice(None)
                copies.append((results[index].at[pick], outs[index].at[pick]))
            for which in range(3):
                copies.append((results[4 + index].at[which], outs[4 + 4 * which + index]))
        copies = [pltpu.make_async_copy(source, target, sem.at[index]) for index, (source, target) in enumerate(copies)]
        for copy in copies:
            copy.start()
        for copy in copies:
            copy.wait()

    def local_step(*banks):
        grad_attn, grad_mlp, grad_wide, grad_vec = banks[0:4]
        given = [[banks[4 + 4 * which + index] for which in range(3)] for index in range(4)]
        given[3] = [state.T for state in given[3]]
        bits = (2,) * 5
        grad_attn = grad_attn.reshape(2, 8, 32, 8192).transpose(0, 2, 1, 3).reshape(2, *bits, 8, 8192)
        grad_mlp = grad_mlp.reshape(8, 32, 32768).transpose(1, 0, 2).reshape(1, *bits, 8, 32768)
        anywhere = pl.BlockSpec(memory_space=pl.ANY)
        vmem = pl.BlockSpec(memory_space=pltpu.VMEM)
        narrow, wide = jnp.bfloat16, jnp.float32
        scratch = []
        streams = make_streams()
        for stream in streams:
            scratch += stream.scratch()
        small = [
            ((LANES, LANES), wide), ((DEVICES, HALF, LANES), narrow), ((DEVICES, HALF, LANES), narrow), ((DEVICES, 4, LANES), narrow),
            ((2, *TILE), wide), ((HALF, LANES), wide), ((4, LANES), wide), ((HALF, LANES), narrow), ((4, LANES), narrow),
            ((DEVICES, HALF, LANES), narrow), ((DEVICES, 4, LANES), narrow), ((HALF, LANES), wide), (grad_wide.shape[1:], narrow), (grad_vec.shape[1:], narrow),
            ((1, LANES), wide), ((DEVICES, 1, LANES), wide), (TILE, wide), ((DEVICES, *TILE), wide), (TILE, wide),
            ((2, HALF, LANES), wide), ((2, *TILE), wide),
        ]
        scratch += [pltpu.VMEM(*spec) for spec in small] + [pltpu.SemaphoreType.DMA] * 14
        replicas = [(grad_attn.shape, narrow), (grad_mlp.shape, narrow), (grad_wide.shape[1:], narrow), (grad_vec.shape[1:], narrow)]
        states = [((3, *state[0].shape), wide) for state in given]
        results = pl.pallas_call(
            kernel,
            name="lamb",
            out_shape=[pltpu.VMEM(*spec) for spec in replicas + states],
            in_specs=[anywhere] * 16,
            out_specs=[vmem] * 8,
            scratch_shapes=scratch,
            compiler_params=pltpu.CompilerParams(has_side_effects=True, collective_id=0, vmem_limit_bytes=32 * 2 ** 20),
        )(grad_attn, grad_mlp, grad_wide, grad_vec, *[state for bank in given for state in bank])
        shape = jax.ShapeDtypeStruct
        outs = list(pl.pallas_call(
            store,
            name="store",
            out_shape=[shape(*spec) for spec in replicas] + [shape(spec[0][1:], wide) for spec in states] * 3,
            in_specs=[vmem] * 8,
            out_specs=[anywhere] * 16,
            scratch_shapes=[pltpu.SemaphoreType.DMA((22,))],
            compiler_params=pltpu.CompilerParams(vmem_limit_bytes=2 ** 20),
        )(*results))
        outs[0] = outs[0].reshape(2, 32, 8, 8192).transpose(0, 2, 1, 3).reshape(16, -1)
        outs[1] = outs[1].reshape(32, 8, 32768).transpose(1, 0, 2).reshape(8, -1)
        for index in (7, 11, 15):
            outs[index] = outs[index].T
        return tuple(outs)

    return jax.shard_map(local_step, mesh=mesh, in_specs=(grad_spec,) * 4 + (shard_spec,) * 12, out_specs=(full_spec,) * 4 + (shard_spec,) * 12, check_vma=False)
```

```python
import jax
import jax.numpy as jnp
from jax import lax
from jax.sharding import PartitionSpec as P
from jax.experimental import pallas as pl
from jax.experimental.pallas import tpu as pltpu

STEP_NUMBER = 10
LEARN_RATE = 0.04
BETA_FIRST = 0.9
BETA_SECOND = 0.999
EPSILON = 1e-6
WEIGHT_DECAY = 0.01
MAX_NORM = 1.0

AHEAD = 1
SLOTS = AHEAD + 1
SCRATCHES = 14
DEVICES, HALF, OTHERS = 32, 16, 31
LANES = 128
VECTORS = 38
TILE = (8, 128)
CORE, X, Y, Z0, Z1 = 1, 2, 4, 8, 16
ROUTES = (
    ("attn", (Z0, X, Y, Z1), 0),
    ("mlp", (X, Y, Z0, Z1), 0),
    ("mlp", (Y, X, Z0, Z1), 12288),
)
GROUPS = ((16,(4,6,10)),)
NATURAL = (Z1, Z0, Y, X, CORE)
ROWS = {"attn": 16, "mlp": 8}
SHARD = {"attn": 8192, "mlp": 32768}
MESH = pl.DeviceIdType.MESH
HIGHEST = lax.Precision.HIGHEST


def loop(first, stop, body):
    lax.fori_loop(first, stop, body, 0)


def direction(grad, weight, first, second, clip):
    clipped = clip * grad
    new_first = BETA_FIRST * first + (1.0 - BETA_FIRST) * clipped
    new_second = BETA_SECOND * second + (1.0 - BETA_SECOND) * (clipped * clipped)
    update = (new_first / (1.0 - BETA_FIRST ** STEP_NUMBER)) / (jnp.sqrt(new_second / (1.0 - BETA_SECOND ** STEP_NUMBER)) + EPSILON) + WEIGHT_DECAY * weight
    return update, new_first, new_second


def fold_lanes(value):
    total = value[:, 0:LANES]
    for column in range(LANES, value.shape[1], LANES):
        total = total + value[:, column:column + LANES]
    return total


TOTAL = sum(chunks for chunks, _ in GROUPS)


class Stream:
    def __init__(self, bank, order, first_column, width, chunks, begin, gather_begin):
        self.bank, self.order, self.first_column, self.width, self.chunks = bank, order, first_column, width, chunks
        self.columns, self.begin, self.gather_begin = width * chunks, begin, gather_begin
        self.reduce_order = (order[0], CORE) + order[1:]
        self.rows = ROWS[bank]
        self.tiles = self.rows // 8
        self.kept_dims = [weight for weight in NATURAL if weight != order[0]]

    def scratch(self):
        rows, width = self.rows, self.width
        return [
            pltpu.VMEM((SLOTS, self.tiles, 2, 2, 2, 2, 8, width), jnp.bfloat16),
            pltpu.VMEM((2, 16, rows, width), jnp.float32),
            pltpu.VMEM((self.chunks, 8, rows, width), jnp.float32),
            pltpu.VMEM((self.chunks, 4, rows, width), jnp.float32),
            pltpu.VMEM((self.chunks, 2, rows, width), jnp.float32),
            pltpu.VMEM((self.chunks, 1, rows, width), jnp.float32),
            pltpu.SemaphoreType.DMA((SLOTS,)),
            pltpu.SemaphoreType.DMA((2,)),
            pltpu.SemaphoreType.DMA((5, self.chunks)),
            pltpu.SemaphoreType.DMA((5,)),
            pltpu.SemaphoreType.DMA((4, self.chunks)),
            pltpu.SemaphoreType.DMA((4,)),
            pltpu.SemaphoreType.DMA,
            pltpu.SemaphoreType.DMA,
        ]

    def bind(self, refs, replica, state):
        self.replica, self.state = replica, state
        (self.own, self.acc, self.part8, self.part4, self.part2, self.part1,
         self.own_sem, self.core_send, self.recv, self.send, self.gather_recv, self.gather_sent, self.core_sent, self.core_got) = refs


def make_streams():
    streams, begin = [], 0
    firsts = [route[2] for route in ROUTES]
    for chunks, tiles in GROUPS:
        for index, (bank, order, _) in enumerate(ROUTES):
            width = tiles[index] * LANES
            streams.append(Stream(bank, order, firsts[index], width, chunks, begin, TOTAL - begin - chunks))
            firsts[index] += width * chunks
        begin += chunks
    return streams


def solution(mesh):
    grad_spec = P("data", None, None)
    shard_spec = P(None, "data")
    full_spec = P(None, None)

    def kernel(*refs):
        grads = {"attn": refs[0], "mlp": refs[1]}
        given_wide_grad, given_vec_grad = refs[2:4]
        given_states = {"attn": refs[4:7], "mlp": refs[7:10]}
        given_wide, given_vec = refs[10:13], refs[13:16]
        replicas = {"attn": refs[16], "mlp": refs[17]}
        replica_wide, replica_vec = refs[18:20]
        states = {"attn": refs[20], "mlp": refs[21]}
        state_wide, state_vec = refs[22:24]
        rest = refs[24:]
        streams = make_streams()
        for index, stream in enumerate(streams):
            stream.bind(rest[SCRATCHES * index:SCRATCHES * (index + 1)], replicas[stream.bank], states[stream.bank])
        (square_pad, vec_rows, vec_land, wide_land, vec_sums, vec_pack, wide_pack, vec_out, wide_out, vec_got, wide_got, vec_grad, grad_wide, grad_vec,
         norm_out, norm_land, tile_out, tile_land, square, row_attn, row_mlp,
         vec_send, vec_recv, wide_send, wide_recv, norm_send, norm_recv, tile_send, tile_recv,
         vec_sent, vec_back, wide_sent, wide_back, load_sem, grad_sem) = rest[SCRATCHES * len(streams):]

        me = lax.axis_index("data")
        bit = {w: (me // w) % 2 for w in (CORE, X, Y, Z0, Z1)}
        peer = {w: me + w - 2 * w * bit[w] for w in bit}

        def blocks(s, whole, columns, fixed):
            picks = [fixed.get(weight, slice(None)) for weight in NATURAL]
            return whole.at[(slice(None), *picks, slice(None), columns)]

        def chunk(s, k):
            start = s.first_column + k * s.width
            return pl.ds(start if isinstance(k, int) else pl.multiple_of(start, LANES), s.width)

        def every(s):
            return pl.ds(s.first_column, s.columns)

        def remote(src, dst, send_sem, recv_sem, device):
            return pltpu.make_async_remote_copy(src_ref=src, dst_ref=dst, send_sem=send_sem, recv_sem=recv_sem, device_id=(device,), device_id_type=MESH)

        def local(src, dst, sem):
            return pltpu.make_async_copy(src, dst, sem)

        def start_raw(s, k):
            slot = k % SLOTS
            first = s.order[0]
            given, kept = [{first: value} for value in (1 - bit[first], bit[first])]
            remote(blocks(s, grads[s.bank], chunk(s, k), given), blocks(s, s.replica, chunk(s, k), given), s.send.at[0], s.recv.at[0, k], peer[first]).start()
            local(blocks(s, grads[s.bank], chunk(s, k), kept), s.own.at[slot], s.own_sem.at[slot]).start()

        def add_raw(s, k):
            slot = k % 2
            mine = k % SLOTS
            local(s.own.at[mine], s.own.at[mine], s.own_sem.at[mine]).wait()
            first = s.order[0]
            landed = blocks(s, s.replica, chunk(s, k), {first: bit[first]})
            remote(landed, landed, s.send.at[0], s.recv.at[0, k], peer[first]).wait_recv()

            @pl.when(k >= 2)
            def _():
                remote(s.acc.at[slot, pl.ds(8, 8)], s.part8.at[k], s.core_send.at[slot], s.recv.at[1, k], peer[CORE]).wait_send()

            def add_block(high, low):
                place = {first: bit[first]}
                for bits, weights in ((high, (CORE, s.order[1])), (low, s.order[2:])):
                    for shift, weight in ((2, weights[0]), (1, weights[1])):
                        place[weight] = (bit[weight] + bits // shift) % 2
                kept = [place[weight] for weight in s.kept_dims]
                owner = [place[weight] for weight in NATURAL]
                for tile in range(s.tiles):
                    got = s.replica[(tile, *owner, slice(None), chunk(s, k))]
                    s.acc[slot, 4 * high + low, 8 * tile:8 * tile + 8] = s.own[(mine, tile, *kept)].astype(jnp.float32) + got.astype(jnp.float32)

            def body(high, carry):
                for low in range(4):
                    add_block(high, low)
                return carry

            loop(2, 4, body)
            remote(s.acc.at[slot, pl.ds(8, 8)], s.part8.at[k], s.core_send.at[slot], s.recv.at[1, k], peer[CORE]).start()
            loop(0, 2, body)

        def add_core(s, k):
            slot = k % 2
            remote(s.acc.at[slot, pl.ds(8, 8)], s.part8.at[k], s.core_send.at[slot], s.recv.at[1, k], peer[CORE]).wait_recv()

            def body(rel, carry):
                s.part8[k, rel] = s.part8[k, rel] + s.acc[slot, rel]
                return carry

            loop(4, 8, body)
            remote(s.part8.at[k, pl.ds(4, 4)], s.part4.at[k], s.send.at[2], s.recv.at[2, k], peer[s.order[1]]).start()
            loop(0, 4, body)

        def add_step(s, k, stage):
            held, got = (s.part8, s.part4) if stage == 2 else (s.part4, s.part2)
            half = 4 if stage == 2 else 2
            nxt = s.part2 if stage == 2 else s.part1
            remote(held.at[k, pl.ds(half, half)], got.at[k], s.send.at[stage], s.recv.at[stage, k], peer[s.order[stage - 1]]).wait_recv()

            def body(rel, carry):
                got[k, rel] = got[k, rel] + held[k, rel]
                return carry

            quarter = half // 2
            loop(quarter, half, body)
            remote(got.at[k, pl.ds(quarter, quarter)], nxt.at[k], s.send.at[stage + 1], s.recv.at[stage + 1, k], peer[s.order[stage]]).start()
            loop(0, quarter, body)

        def add_last(s, k):
            remote(s.part2.at[k, pl.ds(1, 1)], s.part1.at[k], s.send.at[4], s.recv.at[4, k], peer[s.order[3]]).wait_recv()
            grad = (s.part1[k, 0] + s.part2[k, 0]) * (1.0 / 32.0)
            s.part1[k, 0] = grad
            part = fold_lanes(grad * grad)
            for row in range(0, s.rows, 8):
                square[...] += part[row:row + 8]

        def at(chosen, time, begin, act):
            for first in sorted({getattr(s, begin) for s in chosen}):
                group = [s for s in chosen if getattr(s, begin) == first]
                k = time - first

                def run(group=group, k=k):
                    for s in group:
                        act(s, k)

                if isinstance(k, int):
                    if 0 <= k < group[0].chunks:
                        run()
                else:
                    pl.when(jnp.logical_and(k >= 0, k < group[0].chunks))(run)

        def to_all(block_for, land, send_sem, recv_sem):
            def body(d, carry):
                other = (me + d) % DEVICES
                remote(block_for(other), land.at[me], send_sem, recv_sem, other).start()
                return carry

            loop(1, DEVICES, body)

        def from_all(land, send_sem, recv_sem):
            blocks = land.at[pl.ds(0, OTHERS)]
            return remote(blocks, blocks, send_sem, recv_sem, me)

        barrier = pltpu.get_barrier_semaphore()
        for weight in NATURAL:
            pl.semaphore_signal(barrier, inc=1, device_id=(peer[weight],), device_id_type=MESH)
        pl.semaphore_wait(barrier, len(NATURAL))
        for t in range(AHEAD):
            at(streams, t, "begin", start_raw)
        local(given_wide_grad.at[0], grad_wide, grad_sem).start()
        local(given_vec_grad.at[0], grad_vec, grad_sem).start()
        for bank in states:
            for which in range(3):
                local(given_states[bank][which], states[bank].at[which], load_sem).start()
        for which in range(3):
            local(given_wide[which], state_wide.at[which], load_sem).start()
            local(given_vec[which], state_vec.at[which], load_sem).start()

        def turned(z):
            return pl.ds(z * LANES, LANES)

        local(grad_wide, grad_wide, grad_sem).wait()
        local(grad_vec, grad_vec, grad_sem).wait()
        square_pad[...] = jnp.zeros_like(square_pad)
        for z in range(4):
            square_pad[0:VECTORS] = grad_vec[:, turned(z)].astype(jnp.float32)
            rows = square_pad[...].T.astype(jnp.bfloat16)
            for place in range(8):
                vec_rows[8 * z + place] = rows[16 * place:16 * place + 16]

        def wide_tile(owner):
            return pl.ds(pl.multiple_of(owner // 2 * LANES, LANES), LANES)

        vec_land[me] = vec_rows[me]
        wide_land[me] = grad_wide[:, wide_tile(me)]
        def start_small():
            to_all(lambda other: vec_rows.at[other], vec_land, vec_send, vec_recv)
            to_all(lambda other: grad_wide.at[:, wide_tile(other)], wide_land, wide_send, wide_recv)

        square[...] = jnp.zeros_like(square)

        stages = (add_raw, add_core, lambda s, k: add_step(s, k, 2), lambda s, k: add_step(s, k, 3), add_last)

        def reduce_step(t, carry):
            at(streams, t + AHEAD, "begin", start_raw)
            for lag in range(len(stages)):
                at(streams, t - lag, "begin", stages[lag])
            return carry

        loop(0, TOTAL // 2, reduce_step)
        start_small()
        loop(TOTAL // 2, TOTAL, reduce_step)

        from_all(vec_land, vec_send, vec_recv).wait_recv()
        from_all(wide_land, wide_send, wide_recv).wait_recv()

        def sum_all(land):
            total = land[0].astype(jnp.float32)
            for d in range(1, DEVICES):
                total = total + land[d].astype(jnp.float32)
            return total

        vec_full = sum_all(vec_land) * (1.0 / 32.0)
        wide_full = sum_all(wide_land) * (1.0 / 32.0)
        wide_full = jnp.where(bit[CORE] == 0, wide_full, pltpu.roll(wide_full, 64, 1))
        lane_wide = lax.broadcasted_iota(jnp.int32, (4, LANES), 1)
        wide_full = jnp.where(lane_wide < 64, wide_full, 0.0)
        vec_grad[...] = vec_full
        wide_pack[...] = wide_full
        square[0:1] += jnp.sum(vec_full * vec_full, axis=0, keepdims=True) + jnp.sum(wide_full * wide_full, axis=0, keepdims=True)

        loop(TOTAL, TOTAL + len(stages) - 1, reduce_step)

        norm_out[...] = jnp.sum(square[...], axis=0, keepdims=True)
        norm_land[me] = norm_out[...]

        to_all(lambda other: norm_out, norm_land, norm_send, norm_recv)

        for state in (states["attn"], states["mlp"], state_wide, state_vec):
            local(state, state, load_sem).wait()
        row_attn[...] = jnp.zeros_like(row_attn)
        row_mlp[...] = jnp.zeros_like(row_mlp)
        rows_of = {"attn": row_attn, "mlp": row_mlp}
        for s in streams:
            def weight_rows(k, carry, s=s):
                weight = s.state[0, :, chunk(s, k)]
                rows_of[s.bank][1] += fold_lanes(weight * weight)
                return carry
            loop(0, s.chunks, weight_rows)

        from_all(norm_land, norm_send, norm_recv).wait_recv()
        total = jnp.zeros((1, LANES), jnp.float32)
        for d in range(DEVICES):
            total = total + norm_land[d]
        clip = jnp.minimum(1.0, MAX_NORM / jnp.sqrt(jnp.sum(total, axis=1, keepdims=True)))

        for s in streams:
            def move(k, carry, s=s):
                here = chunk(s, k)
                update, new_first, new_second = direction(s.part1[k, 0], *[s.state[which, :, here] for which in range(3)], clip)
                s.part1[k, 0] = update
                s.state[1, :, here] = new_first
                s.state[2, :, here] = new_second
                rows_of[s.bank][0] += fold_lanes(update * update)
                return carry
            loop(0, s.chunks, move)
        vec_weight, wide_weight = state_vec[0], state_wide[0]
        vec_update, state_vec[1], state_vec[2] = direction(vec_grad[:, 0:VECTORS], vec_weight, state_vec[1], state_vec[2], clip)
        wide_update, state_wide[1], state_wide[2] = direction(wide_pack[:, 0:64], wide_weight, state_wide[1], state_wide[2], clip)
        vec_pack[...] = jnp.zeros_like(vec_pack)
        for which, value in enumerate((vec_update, vec_weight)):
            vec_pack[0:1, 0:VECTORS] = jnp.sum(value * value, axis=0, keepdims=True)
            vec_sums[which] = pltpu.roll(vec_pack[0:8], 64, 1)

        lane = lax.broadcasted_iota(jnp.int32, TILE, 1)
        row = lax.broadcasted_iota(jnp.int32, TILE, 0)
        tile = vec_sums[0] + pltpu.roll(vec_sums[1], 1, 0)
        wide_sums = [jnp.sum(value * value, axis=1, keepdims=True) for value in (wide_update, wide_weight)]
        wide_pack[...] = jnp.where(lane_wide == 3, wide_sums[0], 0.0) + jnp.where(lane_wide == 19, wide_sums[1], 0.0)
        tile_out[...] = tile
        tile_out[0:4] += wide_pack[...]
        tile = tile_out[...]
        for which, base in ((0, 0), (1, 16)):
            attn_sum = jnp.sum(row_attn[which], axis=1, keepdims=True)
            mlp_sum = jnp.sum(row_mlp[which], axis=1, keepdims=True)
            tile = tile + jnp.where(lane == base, attn_sum[0:8], 0.0) + jnp.where(lane == base + 1, attn_sum[8:16], 0.0) + jnp.where(lane == base + 2, mlp_sum, 0.0)
        tile_out[...] = tile
        tile_land[me] = tile

        to_all(lambda other: tile_out, tile_land, tile_send, tile_recv)

        from_all(tile_land, tile_send, tile_recv).wait_recv()
        sums = tile_land[0]
        for d in range(1, DEVICES):
            sums = sums + tile_land[d]

        def lane_column(index):
            return jnp.sum(jnp.where(lane == index, sums, 0.0), axis=1, keepdims=True)

        def scale(weight_square, update_square):
            return LEARN_RATE * (jnp.sqrt(weight_square) / jnp.sqrt(update_square))

        scale_attn = jnp.concatenate([scale(lane_column(16), lane_column(0)), scale(lane_column(17), lane_column(1))], axis=0)
        scales = {"attn": scale_attn, "mlp": scale(lane_column(18), lane_column(2))}

        def gathered(s, columns, j, newest=None, core=0):
            fixed = {weight: bit[weight] for weight in s.order[:4 - j]}
            if newest is not None:
                weight = s.order[3 - newest]
                fixed[weight] = 1 - bit[weight]
            fixed[CORE] = (bit[CORE] + core) % 2
            return blocks(s, replicas[s.bank], columns, fixed)

        def gather_send(s, k, j):
            held = gathered(s, chunk(s, k), j)
            remote(held, held, s.gather_sent.at[j], s.gather_recv.at[j, k], peer[s.order[3 - j]]).start()

        def gather_wait(s, k, j):
            got = gathered(s, chunk(s, k), j, j)
            remote(got, got, s.gather_sent.at[j], s.gather_recv.at[j, k], me).wait_recv()

        def core_send(s, k, j):
            got = gathered(s, chunk(s, k), j, j)
            remote(got, got, s.core_sent, s.core_got, peer[CORE]).start()

        def renew(s, k):
            here = chunk(s, k)
            new_weight = s.state[0, :, here] - scales[s.bank] * s.part1[k, 0]
            s.state[0, :, here] = new_weight
            for tile in range(s.tiles):
                s.replica[(tile, *[bit[weight] for weight in NATURAL], slice(None), here)] = new_weight[8 * tile:8 * tile + 8].astype(jnp.bfloat16)

        def first_sends(s, k):
            mine = gathered(s, chunk(s, k), 0)
            gather_send(s, k, 0)
            remote(mine, mine, s.core_sent, s.core_got, peer[CORE]).start()

        def gather_last(s, k):
            gather_wait(s, k, 3)
            core_send(s, k, 3)

        def gather_next(s, k, j):
            gather_wait(s, k, j - 1)
            gather_send(s, k, j)
            core_send(s, k, j - 1)

        def gather_step(t, carry):
            at(streams, t, "gather_begin", renew)
            at(streams, t, "gather_begin", first_sends)
            for j in (1, 2, 3):
                at(streams, t - j, "gather_begin", lambda s, k, j=j: gather_next(s, k, j))
            at(streams, t - 4, "gather_begin", gather_last)
            return carry

        loop(0, TOTAL // 2, gather_step)

        turned_sums = pltpu.roll(jnp.where(row < 2, sums, 1.0), 64, 1)
        scale_vec = scale(turned_sums[1:2, 0:VECTORS], turned_sums[0:1, 0:VECTORS])
        vec_new = vec_weight - scale_vec * vec_update
        wide_new = wide_weight - scale(lane_column(19)[0:4], lane_column(3)[0:4]) * wide_update
        state_vec[0] = vec_new
        state_wide[0] = wide_new
        vec_pack[:, 0:VECTORS] = vec_new
        vec_out[...] = vec_pack[...].astype(jnp.bfloat16)
        wide_pack[...] = jnp.zeros_like(wide_pack)
        wide_pack[:, 0:64] = wide_new
        wide_out[...] = (wide_pack[...] + pltpu.roll(wide_pack[...], 64, 1)).astype(jnp.bfloat16)
        vec_got[me] = vec_out[...]
        wide_got[me] = wide_out[...]
        to_all(lambda other: vec_out, vec_got, vec_sent, vec_back)
        to_all(lambda other: wide_out, wide_got, wide_sent, wide_back)
        loop(TOTAL // 2, TOTAL, gather_step)

        from_all(vec_got, vec_sent, vec_back).wait()
        from_all(wide_got, wide_sent, wide_back).wait()
        for z in range(4):
            for place in range(8):
                square_pad[16 * place:16 * place + 16] = vec_got[8 * z + place].astype(jnp.float32)
            replica_vec[:, turned(z)] = square_pad[...].T[0:VECTORS].astype(jnp.bfloat16)
        for pair in range(HALF):
            low, high = wide_got[2 * pair].astype(jnp.float32), wide_got[2 * pair + 1].astype(jnp.float32)
            replica_wide[:, turned(pair)] = jnp.where(lane_wide < 64, low, high).astype(jnp.bfloat16)

        loop(TOTAL, TOTAL + 4, gather_step)

        for s in streams:
            half = gathered(s, every(s), 4)
            remote(half, half, s.core_sent, s.core_got, me).wait()
            for j in range(4):
                held = gathered(s, every(s), j)
                remote(held, held, s.gather_sent.at[j], s.core_got, me).wait_send()
            first = s.order[0]
            landed = blocks(s, s.replica, every(s), {first: bit[first]})
            remote(landed, landed, s.send.at[0], s.recv.at[0, 0], me).wait_send()
            for last in range(s.chunks - 2, s.chunks):
                slot = last % 2
                remote(s.acc.at[slot, pl.ds(8, 8)], s.part8.at[last], s.core_send.at[slot], s.recv.at[1, last], me).wait_send()
            for stage, part in ((2, s.part4), (3, s.part2), (4, s.part1)):
                remote(part, part, s.send.at[stage], s.recv.at[0, 0], me).wait_send()
        from_all(vec_land, vec_send, vec_recv).wait_send()
        from_all(wide_land, wide_send, wide_recv).wait_send()
        from_all(norm_land, norm_send, norm_recv).wait_send()
        from_all(tile_land, tile_send, tile_recv).wait_send()

    def store(*refs):
        results, outs, sem = refs[:8], refs[8:24], refs[24]
        copies = []
        for index in range(4):
            parts = [(z1, z0) for z1 in range(2) for z0 in range(2)] if index < 2 else [None]
            for part in parts:
                pick = (slice(None), *part) if part else slice(None)
                copies.append((results[index].at[pick], outs[index].at[pick]))
            for which in range(3):
                copies.append((results[4 + index].at[which], outs[4 + 4 * which + index]))
        copies = [pltpu.make_async_copy(source, target, sem.at[index]) for index, (source, target) in enumerate(copies)]
        for copy in copies:
            copy.start()
        for copy in copies:
            copy.wait()

    def local_step(*banks):
        grad_attn, grad_mlp, grad_wide, grad_vec = banks[0:4]
        given = [[banks[4 + 4 * which + index] for which in range(3)] for index in range(4)]
        given[3] = [state.T for state in given[3]]
        bits = (2,) * 5
        grad_attn = grad_attn.reshape(2, 8, 32, 8192).transpose(0, 2, 1, 3).reshape(2, *bits, 8, 8192)
        grad_mlp = grad_mlp.reshape(8, 32, 32768).transpose(1, 0, 2).reshape(1, *bits, 8, 32768)
        anywhere = pl.BlockSpec(memory_space=pl.ANY)
        vmem = pl.BlockSpec(memory_space=pltpu.VMEM)
        narrow, wide = jnp.bfloat16, jnp.float32
        scratch = []
        streams = make_streams()
        for stream in streams:
            scratch += stream.scratch()
        small = [
            ((LANES, LANES), wide), ((DEVICES, HALF, LANES), narrow), ((DEVICES, HALF, LANES), narrow), ((DEVICES, 4, LANES), narrow),
            ((2, *TILE), wide), ((HALF, LANES), wide), ((4, LANES), wide), ((HALF, LANES), narrow), ((4, LANES), narrow),
            ((DEVICES, HALF, LANES), narrow), ((DEVICES, 4, LANES), narrow), ((HALF, LANES), wide), (grad_wide.shape[1:], narrow), (grad_vec.shape[1:], narrow),
            ((1, LANES), wide), ((DEVICES, 1, LANES), wide), (TILE, wide), ((DEVICES, *TILE), wide), (TILE, wide),
            ((2, HALF, LANES), wide), ((2, *TILE), wide),
        ]
        scratch += [pltpu.VMEM(*spec) for spec in small] + [pltpu.SemaphoreType.DMA] * 14
        replicas = [(grad_attn.shape, narrow), (grad_mlp.shape, narrow), (grad_wide.shape[1:], narrow), (grad_vec.shape[1:], narrow)]
        states = [((3, *state[0].shape), wide) for state in given]
        results = pl.pallas_call(
            kernel,
            name="lamb",
            out_shape=[pltpu.VMEM(*spec) for spec in replicas + states],
            in_specs=[anywhere] * 16,
            out_specs=[vmem] * 8,
            scratch_shapes=scratch,
            compiler_params=pltpu.CompilerParams(has_side_effects=True, collective_id=0, vmem_limit_bytes=32 * 2 ** 20),
        )(grad_attn, grad_mlp, grad_wide, grad_vec, *[state for bank in given for state in bank])
        shape = jax.ShapeDtypeStruct
        outs = list(pl.pallas_call(
            store,
            name="store",
            out_shape=[shape(*spec) for spec in replicas] + [shape(spec[0][1:], wide) for spec in states] * 3,
            in_specs=[vmem] * 8,
            out_specs=[anywhere] * 16,
            scratch_shapes=[pltpu.SemaphoreType.DMA((22,))],
            compiler_params=pltpu.CompilerParams(vmem_limit_bytes=2 ** 20),
        )(*results))
        outs[0] = outs[0].reshape(2, 32, 8, 8192).transpose(0, 2, 1, 3).reshape(16, -1)
        outs[1] = outs[1].reshape(32, 8, 32768).transpose(1, 0, 2).reshape(8, -1)
        for index in (7, 11, 15):
            outs[index] = outs[index].T
        return tuple(outs)

    return jax.shard_map(local_step, mesh=mesh, in_specs=(grad_spec,) * 4 + (shard_spec,) * 12, out_specs=(full_spec,) * 4 + (shard_spec,) * 12, check_vma=False)
```
